8 devices in a mesh: data: 2 (over z, y), stage: 4 (over x, core).
Axes of the slice: x: 2, y: 2, z: 1, core: 2. Of those that a mesh axis runs over, the one named last changes fastest.
Arguments:
- x_init: float32 [64, 64, 64], P('data'), parts along dimension 0
- h_warm: bfloat16 [3, 64, 64, 1024], P(None, 'data'), parts along dimension 1
- w_lat: bfloat16 [4, 64, 1024], P('stage')
- w_qkv: bfloat16 [4, 1024, 3072], P('stage')
- w_o: bfloat16 [4, 16, 64, 1024], P('stage')
- w_up: bfloat16 [4, 1024, 4096], P('stage')
- w_down: bfloat16 [4, 4096, 1024], P('stage')
- w_out: bfloat16 [1024, 64], replicated
- ada_mods: float32 [4, 4, 6, 1024], P(None, 'stage')
- alpha_coef: float32 [4], replicated
- beta_coef: float32 [4], replicated
Outputs:
- output 1: float32 [64, 64, 64], P('data'), parts along dimension 0
- output 2: bfloat16 [4, 64, 64, 1024], P('stage', 'data'), parts along dimension 1
There are 2 independent parts. The reference program is written for one: setup_inputs(seed, part) draws one part's arguments, and reference() takes and returns one part's arrays. A program takes and returns all parts, laid end to end along the dimension named above; an argument that names none is the same for every part.
All inputs are finite; a program needn't handle non-finite values.
Results may differ from the reference program's by a relative error of at most 0.02.
Values are sent between devices in bfloat16 or wider.
A program may use at most 1 GiB of HBM per device.

```python
import jax
import jax.numpy as jnp
from jax import lax

D = 1024
HEADS = 16
TOKENS = 64
CH = 64
BATCH = 32
BLOCKS_STAGE = 1
STEPS = 4
STAGES = 4

LAYERS = STAGES * BLOCKS_STAGE
HEAD = D // HEADS


def setup_inputs(seed: int = 0, part: int = 0) -> dict:
    shared_keys = jax.random.split(jax.random.key(seed), 9)
    part_keys = jax.random.split(jax.random.fold_in(jax.random.key(seed + 1), part), 2)
    x_init = jax.random.normal(part_keys[0], (BATCH, TOKENS, CH), jnp.float32)
    h_warm = jax.random.normal(part_keys[1], (STAGES - 1, BATCH, TOKENS, D), jnp.float32).astype(jnp.bfloat16)
    w_lat = (jax.random.normal(shared_keys[0], (STAGES, CH, D), jnp.float32) * CH ** -0.5).astype(jnp.bfloat16)
    w_qkv = (jax.random.normal(shared_keys[1], (LAYERS, D, 3 * D), jnp.float32) * (1.5 * D ** -0.5)).astype(jnp.bfloat16)
    w_o = (jax.random.normal(shared_keys[2], (LAYERS, HEADS, HEAD, D), jnp.float32) * D ** -0.5).astype(jnp.bfloat16)
    w_up = (jax.random.normal(shared_keys[3], (LAYERS, D, 4 * D), jnp.float32) * D ** -0.5).astype(jnp.bfloat16)
    w_down = (jax.random.normal(shared_keys[4], (LAYERS, 4 * D, D), jnp.float32) * (4 * D) ** -0.5).astype(jnp.bfloat16)
    w_out = (jax.random.normal(shared_keys[5], (D, CH), jnp.float32) * D ** -0.5).astype(jnp.bfloat16)
    mod_base = jnp.array([0.0, 0.0, 1.0, 0.0, 0.0, 0.6], jnp.float32)[:, None]
    ada_mods = mod_base + 0.3 * jax.random.normal(shared_keys[6], (STEPS, LAYERS, 6, D), jnp.float32)
    alpha_coef = jax.random.uniform(shared_keys[7], (STEPS,), jnp.float32, 0.7, 1.0)
    beta_coef = -jax.random.uniform(shared_keys[8], (STEPS,), jnp.float32, 0.3, 0.6)
    return {'x_init': x_init, 'h_warm': h_warm, 'w_lat': w_lat, 'w_qkv': w_qkv, 'w_o': w_o, 'w_up': w_up, 'w_down': w_down, 'w_out': w_out, 'ada_mods': ada_mods, 'alpha_coef': alpha_coef, 'beta_coef': beta_coef}


def layer_norm(h_cur):
    row_mean = jnp.mean(h_cur, axis=-1, keepdims=True)
    centered = h_cur - row_mean
    row_var = jnp.mean(centered * centered, axis=-1, keepdims=True)
    return centered * lax.rsqrt(row_var + 1e-6)


def dit_block(h_cur, w_qkv, w_o, w_up, w_down, mod_vec):
    batch_size, tokens = h_cur.shape[0], h_cur.shape[1]
    u_attn = (layer_norm(h_cur) * (1.0 + mod_vec[1]) + mod_vec[0]).astype(jnp.bfloat16)
    qkv_proj = jnp.einsum('bnd,de->bne', u_attn.astype(jnp.float32), w_qkv.astype(jnp.float32)).astype(jnp.bfloat16)
    qkv_proj = qkv_proj.reshape(batch_size, tokens, 3, HEADS, HEAD).astype(jnp.float32)
    scores = jnp.einsum('bqhd,bkhd->bhqk', qkv_proj[:, :, 0], qkv_proj[:, :, 1]) * HEAD ** -0.5
    attn_probs = jax.nn.softmax(scores, axis=-1).astype(jnp.bfloat16).astype(jnp.float32)
    attn_out = jnp.einsum('bhqk,bkhd->bqhd', attn_probs, qkv_proj[:, :, 2]).astype(jnp.bfloat16).astype(jnp.float32)
    h_cur = h_cur + mod_vec[2] * jnp.einsum('bqhd,hde->bqe', attn_out, w_o.astype(jnp.float32))
    u_mlp = (layer_norm(h_cur) * (1.0 + mod_vec[4]) + mod_vec[3]).astype(jnp.bfloat16)
    hidden = jax.nn.gelu(jnp.einsum('bnd,df->bnf', u_mlp.astype(jnp.float32), w_up.astype(jnp.float32)), approximate=True).astype(jnp.bfloat16)
    return h_cur + mod_vec[5] * jnp.einsum('bnf,fd->bnd', hidden.astype(jnp.float32), w_down.astype(jnp.float32))


def run_stage(h_cur, weights_s, mods_s):
    def one_block(carry_h, block_in):
        w_qkv, w_o, w_up, w_down, mod_vec = block_in
        return dit_block(carry_h, w_qkv, w_o, w_up, w_down, mod_vec), None
    h_out, _ = lax.scan(one_block, h_cur, weights_s + (mods_s,))
    return h_out


def reference(x_init, h_warm, w_lat, w_qkv, w_o, w_up, w_down, w_out, ada_mods, alpha_coef, beta_coef):
    stage_w = tuple(weight.reshape((STAGES, BLOCKS_STAGE) + weight.shape[1:]) for weight in (w_qkv, w_o, w_up, w_down))
    stage_mods = ada_mods.reshape(STEPS, STAGES, BLOCKS_STAGE, 6, D)
    zero_slot = jnp.zeros((1, BATCH, TOKENS, D), jnp.bfloat16)
    prev_init = jnp.concatenate([h_warm, zero_slot], axis=0)

    def one_step(carry, step_in):
        x_cur, prev_out = carry
        mods_t, alpha_t, beta_t = step_in
        stale_in = jnp.concatenate([zero_slot, prev_out[:-1]], axis=0)
        x_lat = x_cur.astype(jnp.bfloat16).astype(jnp.float32)

        def one_stage(stage_in):
            stale_s, lat_s, weights_s, mods_s = stage_in
            h_cur = stale_s.astype(jnp.float32) + jnp.einsum('bnc,cd->bnd', x_lat, lat_s.astype(jnp.float32))
            return run_stage(h_cur, weights_s, mods_s).astype(jnp.bfloat16)

        stage_out = lax.map(one_stage, (stale_in, w_lat, stage_w, mods_t))
        eps_pred = jnp.einsum('bnd,dc->bnc', stage_out[STAGES - 1].astype(jnp.float32), w_out.astype(jnp.float32))
        x_next = alpha_t * x_cur + beta_t * eps_pred
        return (x_next, stage_out), None

    (x_final, last_out), _ = lax.scan(one_step, (x_init, prev_init), (stage_mods, alpha_coef, beta_coef))
    return x_final, last_out
```

```python
import functools

import jax
import jax.numpy as jnp
from jax import lax
from jax.experimental import pallas as pl
from jax.experimental.pallas import tpu as pltpu
from jax.sharding import PartitionSpec as P

F32, BF16 = jnp.float32, jnp.bfloat16
MESH = pl.DeviceIdType.MESH
D, HEADS, HEAD, TOK, CH, FF = 1024, 16, 64, 64, 64, 4096
ROWS = 256
RB = 16
STAGES = 4
INV_D = 1.0 / D
GC0 = 0.7978845608028654
GC1 = GC0 * 0.044715


def dot(a, b):
    return jnp.dot(a, b, preferred_element_type=F32)


def dot_t(a, b):
    return lax.dot_general(a, b, (((1,), (1,)), ((), ())), preferred_element_type=F32)


def merge(first, second):
    total_a = sum(w for w, _ in first)
    total_b = sum(w for w, _ in second)
    ia = ib = 0
    done_a = done_b = 0.0
    while ia < len(first) or ib < len(second):
        take_a = ib >= len(second) or (ia < len(first) and done_a / total_a <= done_b / total_b)
        if take_a:
            w, piece = first[ia]
            ia, done_a = ia + 1, done_a + w
        else:
            w, piece = second[ib]
            ib, done_b = ib + 1, done_b + w
        piece()


def kernel(steps, chunks,
           x_hbm, warm_hbm, lat_hbm, qkv_hbm, o_hbm, up_hbm, down_hbm, out_hbm, mods_hbm, alpha, beta,
           xout_hbm, hlast_hbm,
           wlat, wk, wqvt, wo, wup, wdown, wout, wtmp, mods,
           buf, xb, xf, ebuf,
           h_a, h_b, u_a, u_b, k_s, qv_s, o_s, hid,
           w_sem, warm_sem, st_send, st_recv, x_send, x_recv, xo_send, xo_recv, xo_loc, hl_sem):
    st = lax.axis_index('stage')
    last = STAGES - 1
    total = steps * chunks

    loads = [
        pltpu.make_async_copy(qkv_hbm.at[:, pl.ds(0, D)], wtmp.at[0], w_sem.at[0]),
        pltpu.make_async_copy(qkv_hbm.at[:, pl.ds(2 * D, D)], wtmp.at[1], w_sem.at[1]),
        pltpu.make_async_copy(x_hbm, xf, w_sem.at[2]),
        pltpu.make_async_copy(mods_hbm, mods, w_sem.at[3]),
        pltpu.make_async_copy(lat_hbm, wlat, w_sem.at[4]),
        pltpu.make_async_copy(qkv_hbm.at[:, pl.ds(D, D)], wk, w_sem.at[5]),
        pltpu.make_async_copy(o_hbm, wo, w_sem.at[6]),
        pltpu.make_async_copy(up_hbm, wup, w_sem.at[7]),
        pltpu.make_async_copy(down_hbm, wdown, w_sem.at[8]),
        pltpu.make_async_copy(out_hbm, wout, w_sem.at[9]),
    ]
    warm_stage = jnp.maximum(st - 1, 0)

    def warm_copy(c):
        return pltpu.make_async_copy(warm_hbm.at[warm_stage, c], buf.at[c], warm_sem.at[c])

    for ld in loads[:5]:
        ld.start()
    warm_copy(0).start()
    for ld in loads[5:]:
        ld.start()
    for c in range(1, chunks):
        warm_copy(c).start()

    barrier = pltpu.get_barrier_semaphore()
    for k in range(1, STAGES):
        pl.semaphore_signal(barrier, inc=1, device_id={'stage': lax.rem(st + k, STAGES)}, device_id_type=MESH)
    pl.semaphore_wait(barrier, STAGES - 1)

    def stale_copy(k):
        nxt = jnp.minimum(st + 1, last)
        return pltpu.make_async_remote_copy(
            src_ref=buf.at[k], dst_ref=buf.at[k + chunks], send_sem=st_send.at[k], recv_sem=st_recv.at[k],
            device_id={'stage': nxt}, device_id_type=MESH)

    def latent_copy(k, dst):
        return pltpu.make_async_remote_copy(
            src_ref=xb.at[k + chunks], dst_ref=xb.at[k + chunks], send_sem=x_send.at[dst, k], recv_sem=x_recv.at[k],
            device_id={'stage': dst}, device_id_type=MESH)

    def xout_copy(c, dst):
        return pltpu.make_async_remote_copy(
            src_ref=xf.at[c], dst_ref=xout_hbm.at[c], send_sem=xo_send.at[dst, c], recv_sem=xo_recv.at[c],
            device_id={'stage': dst}, device_id_type=MESH)

    def hlast_copy(c):
        return pltpu.make_async_copy(buf.at[(steps - 1) * chunks + c], hlast_hbm.at[c], hl_sem.at[c])

    def wait_inputs(k):
        @pl.when(k < chunks)
        def _():
            warm_copy(k).wait()

        @pl.when(jnp.logical_and(k >= chunks, st > 0))
        def _():
            stale_copy(k - chunks).wait_recv()

        @pl.when(jnp.logical_and(k >= chunks, st < last))
        def _():
            latent_copy(k - chunks, 0).wait_recv()

    def send_stage(k):
        @pl.when(jnp.logical_and(k < total - chunks, st < last))
        def _():
            stale_copy(k).start()

        @pl.when(k >= total - chunks)
        def _():
            hlast_copy(k - (total - chunks)).start()

    def finish_latent(k):
        step, c = lax.div(k, chunks), lax.rem(k, chunks)

        @pl.when(st == last)
        def _():
            x_new = alpha[step] * xf[c] + beta[step] * ebuf[...]
            xf[c] = x_new

            @pl.when(step < steps - 1)
            def _():
                xb[k + chunks] = x_new.astype(BF16)
                for dst in range(last):
                    latent_copy(k, dst).start()

            @pl.when(step == steps - 1)
            def _():
                for dst in range(last):
                    xout_copy(c, dst).start()
                pltpu.make_async_copy(xf.at[c], xout_hbm.at[c], xo_loc.at[c]).start()

    lane = lax.broadcasted_iota(jnp.int32, (HEAD, 4 * TOK), 1)
    left = lax.rem(lane, 2 * TOK) < TOK
    zero_q = jnp.zeros((HEAD, 2 * TOK), BF16)

    def norm(h, scale, shift):
        mean = jnp.sum(h, axis=-1, keepdims=True) * INV_D
        cen = h - mean
        var = jnp.sum(cen * cen, axis=-1, keepdims=True) * INV_D
        return (cen * lax.rsqrt(var + 1e-6) * (1.0 + scale) + shift).astype(BF16)

    def a_pieces(k):
        step = lax.div(k, chunks)
        pieces = []

        def latent(n):
            cols = pl.ds(n * 256, 256)
            h_a[:, cols] = dot(xb[k], wlat[:, cols])

        def norm1(r):
            rows = pl.ds(r * RB, RB)
            stale = jnp.where(st > 0, buf[k, rows, :].astype(F32), 0.0)
            h = stale + h_a[rows, :]
            h_a[rows, :] = h
            u_a[rows, :] = norm(h, mods[step, 1:2, :], mods[step, 0:1, :])

        def proj_k(n):
            cols = pl.ds(n * 256, 256)
            k_s[:, cols] = dot(u_a[...], wk[:, cols]).astype(BF16)

        def proj_qv(n):
            rows = pl.ds(n * 512, 512)
            qv_s[rows, :] = dot_t(wqvt[rows, :], u_a[...]).astype(BF16)

        def attend(p, hp):
            r0, l0 = hp * 2 * HEAD, p * 2 * TOK
            q0 = qv_s[r0:r0 + HEAD, l0:l0 + 2 * TOK]
            q1 = qv_s[r0 + HEAD:r0 + 2 * HEAD, l0:l0 + 2 * TOK]
            rhs = jnp.concatenate([jnp.concatenate([q0, zero_q], axis=1), jnp.concatenate([zero_q, q1], axis=1)], axis=0)
            both = dot(k_s[l0:l0 + 2 * TOK, r0:r0 + 2 * HEAD], rhs)
            s = jnp.where(left, both[:TOK], both[TOK:])
            e = jnp.exp((s - jnp.max(s, axis=0, keepdims=True)) * (HEAD ** -0.5))
            pr = e * (1.0 / jnp.sum(e, axis=0, keepdims=True))
            p_l = jnp.where(left, pr, 0.0).astype(BF16)
            p_r = jnp.where(left, 0.0, pr).astype(BF16)
            h2 = 2 * TOK
            rhs = jnp.concatenate([
                jnp.concatenate([p_l[:, :h2], zero_q], axis=1), jnp.concatenate([p_r[:, :h2], zero_q], axis=1),
                jnp.concatenate([zero_q, p_l[:, h2:]], axis=1), jnp.concatenate([zero_q, p_r[:, h2:]], axis=1)], axis=0)
            v = jnp.concatenate([qv_s[D + r0:D + r0 + HEAD, l0:l0 + h2], qv_s[D + r0 + HEAD:D + r0 + 2 * HEAD, l0:l0 + h2]], axis=1)
            ot = dot(v, rhs)
            ot = jnp.concatenate([ot[:, :h2], ot[:, h2:]], axis=0)
            o_s[l0:l0 + h2, r0:r0 + 2 * HEAD] = ot.T.astype(BF16)

        def proj_o(n):
            cols = pl.ds(n * 256, 256)
            h_a[:, cols] = h_a[:, cols] + mods[step, 2:3, n * 256:(n + 1) * 256] * dot(o_s[...], wo[:, cols])

        for n in range(4):
            pieces.append((64, functools.partial(latent, n)))
        for r in range(ROWS // RB):
            pieces.append((40, functools.partial(norm1, r)))
        for n in range(4):
            pieces.append((256, functools.partial(proj_k, n)))
        for n in range(4):
            pieces.append((512, functools.partial(proj_qv, n)))
        for p in range(2):
            for hp in range(HEADS // 2):
                pieces.append((150, functools.partial(attend, p, hp)))
        for n in range(4):
            pieces.append((256, functools.partial(proj_o, n)))
        return pieces

    def norm2_pieces(k):
        step = lax.div(k, chunks)

        def norm2(r):
            rows = pl.ds(r * RB, RB)
            h = h_a[rows, :]
            h_b[rows, :] = h
            u_b[rows, :] = norm(h, mods[step, 4:5, :], mods[step, 3:4, :])

        return [(40, functools.partial(norm2, r)) for r in range(ROWS // RB)]

    def b_pieces(k):
        step = lax.div(k, chunks)
        pieces = []

        def up(n):
            cols = pl.ds(n * 256, 256)
            z = dot(u_b[...], wup[:, cols])
            half = 0.5 * z
            t = jnp.tanh(z * (GC0 + GC1 * (z * z)))
            hid[:, cols] = (half + half * t).astype(BF16)

        def down(n):
            cols = pl.ds(n * 256, 256)
            y = dot(hid[...], wdown[:, cols])
            buf[k, :, cols] = (h_b[:, cols] + mods[step, 5:6, n * 256:(n + 1) * 256] * y).astype(BF16)

        for n in range(FF // 256):
            pieces.append((256, functools.partial(up, n)))
        for n in range(4):
            pieces.append((1024, functools.partial(down, n)))
        return pieces

    def noise(k):
        ebuf[...] = dot(buf[k], wout[...])

    loads[0].wait()
    loads[1].wait()

    @pl.loop(0, D // 128)
    def _(ii):
        sl = pl.ds(pl.multiple_of(ii * 128, 128), 128)
        for part in range(2):
            wqvt[part * D:(part + 1) * D, sl] = wtmp[part, sl, :].T

    for ld in loads[2:7]:
        ld.wait()
    for c in range(chunks):
        xb[c] = xf[c].astype(BF16)
    wait_inputs(0)
    for _, piece in a_pieces(0):
        piece()
    for _, piece in norm2_pieces(0):
        piece()
    for ld in loads[7:]:
        ld.wait()

    @pl.loop(0, total - 1)
    def _(i):
        wait_inputs(i + 1)
        noise(jnp.maximum(i - 1, 0))
        merge(a_pieces(i + 1), b_pieces(i))
        for _, piece in norm2_pieces(i + 1):
            piece()
        send_stage(i)

        @pl.when(i > 0)
        def _():
            finish_latent(i - 1)

    noise(total - 2)
    for _, piece in b_pieces(total - 1):
        piece()
    send_stage(total - 1)
    finish_latent(total - 2)
    noise(total - 1)
    finish_latent(total - 1)

    for c in range(chunks):
        hlast_copy(c).wait()

    @pl.when(st < last)
    def _():
        @pl.loop(0, total - chunks)
        def _(k):
            stale_copy(k).wait_send()

        for c in range(chunks):
            xout_copy(c, 0).wait_recv()

    @pl.when(st == last)
    def _():
        @pl.loop(0, total - chunks)
        def _(k):
            for dst in range(last):
                latent_copy(k, dst).wait_send()

        for c in range(chunks):
            for dst in range(last):
                xout_copy(c, dst).wait_send()
            pltpu.make_async_copy(xf.at[c], xout_hbm.at[c], xo_loc.at[c]).wait()


def solution(mesh):
    def program(x_init, h_warm, w_lat, w_qkv, w_o, w_up, w_down, w_out, ada_mods, alpha_coef, beta_coef):
        batch, steps = x_init.shape[0], ada_mods.shape[0]
        chunks = batch * TOK // ROWS
        total = steps * chunks
        any_spec = pl.BlockSpec(memory_space=pl.ANY)
        smem = pl.BlockSpec(memory_space=pltpu.SMEM)
        dma = pltpu.SemaphoreType.DMA
        flops = 2 * total * ROWS * D * D * 13
        x_out, h_last = pl.pallas_call(
            functools.partial(kernel, steps, chunks),
            out_shape=(jax.ShapeDtypeStruct((chunks, ROWS, CH), F32), jax.ShapeDtypeStruct((chunks, ROWS, D), BF16)),
            in_specs=[any_spec] * 9 + [smem] * 2,
            out_specs=(any_spec, any_spec),
            scratch_shapes=[
                pltpu.VMEM((CH, D), BF16), pltpu.VMEM((D, D), BF16), pltpu.VMEM((2 * D, D), BF16),
                pltpu.VMEM((D, D), BF16), pltpu.VMEM((D, FF), BF16), pltpu.VMEM((FF, D), BF16),
                pltpu.VMEM((D, CH), BF16), pltpu.VMEM((2, D, D), BF16), pltpu.VMEM((steps, 6, D), F32),
                pltpu.VMEM((total, ROWS, D), BF16), pltpu.VMEM((total, ROWS, CH), BF16),
                pltpu.VMEM((chunks, ROWS, CH), F32), pltpu.VMEM((ROWS, CH), F32),
                pltpu.VMEM((ROWS, D), F32), pltpu.VMEM((ROWS, D), F32),
                pltpu.VMEM((ROWS, D), BF16), pltpu.VMEM((ROWS, D), BF16),
                pltpu.VMEM((ROWS, D), BF16), pltpu.VMEM((2 * D, ROWS), BF16), pltpu.VMEM((ROWS, D), BF16),
                pltpu.VMEM((ROWS, FF), BF16),
                dma((10,)), dma((chunks,)), dma((total - chunks,)), dma((total - chunks,)),
                dma((STAGES - 1, total - chunks)), dma((total - chunks,)),
                dma((STAGES - 1, chunks)), dma((chunks,)), dma((chunks,)), dma((chunks,)),
            ],
            compiler_params=pltpu.CompilerParams(
                collective_id=0, has_side_effects=True, vmem_limit_bytes=67_043_328),
            cost_estimate=pl.CostEstimate(flops=flops, bytes_accessed=40 << 20, transcendentals=0),
        )(x_init.reshape(chunks, ROWS, CH), h_warm.reshape(STAGES - 1, chunks, ROWS, D),
          w_lat[0], w_qkv[0], w_o.reshape(D, D), w_up[0], w_down[0], w_out, ada_mods[:, 0], alpha_coef, beta_coef)
        return x_out.reshape(x_init.shape), h_last.reshape(1, batch, TOK, D)

    return jax.shard_map(program, mesh=mesh,
                         in_specs=(P('data'), P(None, 'data'), P('stage'), P('stage'), P('stage'), P('stage'), P('stage'), P(), P(None, 'stage'), P(), P()),
                         out_specs=(P('data'), P('stage', 'data')), check_vma=False)
```

```python
import functools

import jax
import jax.numpy as jnp
from jax import lax
from jax.experimental import pallas as pl
from jax.experimental.pallas import tpu as pltpu
from jax.sharding import PartitionSpec as P

F32, BF16 = jnp.float32, jnp.bfloat16
MESH = pl.DeviceIdType.MESH
D, HEADS, HEAD, TOK, CH, FF = 1024, 16, 64, 64, 64, 4096
ROWS = 256
RB = 16
STAGES = 4
INV_D = 1.0 / D
GC0 = 0.7978845608028654
GC1 = GC0 * 0.044715
LOG2E = 1.4426950408889634
VMEM_LIMIT = 45 << 20


def dot(a, b):
    return jnp.dot(a, b, preferred_element_type=F32)


def dot_t(a, b):
    return lax.dot_general(a, b, (((1,), (1,)), ((), ())), preferred_element_type=F32)


def merge(first, second):
    total_a = sum(w for w, _ in first)
    total_b = sum(w for w, _ in second)
    ia = ib = 0
    done_a = done_b = 0.0
    while ia < len(first) or ib < len(second):
        take_a = ib >= len(second) or (ia < len(first) and done_a / total_a <= done_b / total_b)
        if take_a:
            w, piece = first[ia]
            ia, done_a = ia + 1, done_a + w
        else:
            w, piece = second[ib]
            ib, done_b = ib + 1, done_b + w
        piece()


def wide(ref, rows=slice(None), tiles=None):
    tiles = range(ref.shape[0]) if tiles is None else tiles
    return jnp.concatenate([ref[c, rows, :] for c in tiles], axis=1)


def put(ref, first, rows, value):
    for c in range(value.shape[1] // 128):
        ref[first + c, rows, :] = value[:, c * 128:(c + 1) * 128].astype(BF16)


def kernel(steps, chunks,
           x_hbm, warm_hbm, lat_hbm, qkv_hbm, o_hbm, up_hbm, down_hbm, out_hbm, mods_hbm, alpha, beta,
           xf, buf,
           wlat, wk, wqvt, wo, wup, wdown, wout_t, wout, wtmp, mods_t, mods,
           xb, ebuf,
           h_l, h_a, h_n, h_b, u_a, u_b, k_s, qv_s, o_s, hid,
           q_sem, s_sem, lat_sem, k_sem, o_sem, up_sem, down_sem,
           warm_sem, st_send, st_recv, x_send, x_recv, xo_send, xo_recv):
    st = lax.axis_index('stage')
    last = STAGES - 1
    total = steps * chunks

    def tiled(src, first, dst, sem):
        return [pltpu.make_async_copy(src.at[:, pl.ds(first + c * 128, 128)], dst.at[c], sem.at[c]) for c in range(dst.shape[0])]

    ld_q = [pltpu.make_async_copy(qkv_hbm.at[:, pl.ds(part * 2 * D, D)], wtmp.at[part], q_sem.at[part]) for part in range(2)]
    ld_s = [pltpu.make_async_copy(src, dst, s_sem.at[n])
            for n, (src, dst) in enumerate(((x_hbm, xf), (mods_hbm, mods_t), (out_hbm, wout_t)))]
    ld_lat = tiled(lat_hbm, 0, wlat, lat_sem)
    ld_k = tiled(qkv_hbm, D, wk, k_sem)
    ld_o = tiled(o_hbm, 0, wo, o_sem)
    ld_up = tiled(up_hbm, 0, wup, up_sem)
    ld_down = tiled(down_hbm, 0, wdown, down_sem)
    warm_stage = jnp.maximum(st - 1, 0)

    def warm_copy(c):
        return pltpu.make_async_copy(warm_hbm.at[warm_stage, c], buf.at[c], warm_sem.at[c])

    for ld in ld_q + ld_s + ld_lat:
        ld.start()
    warm_copy(0).start()
    for ld in ld_k + ld_o:
        ld.start()
    warm_copy(1).start()
    for ld in ld_up + ld_down:
        ld.start()
    for c in range(2, chunks):
        warm_copy(c).start()

    barrier = pltpu.get_barrier_semaphore()
    for k in range(1, STAGES):
        pl.semaphore_signal(barrier, inc=1, device_id={'stage': lax.rem(st + k, STAGES)}, device_id_type=MESH)
    pl.semaphore_wait(barrier, STAGES - 1)

    def stale_copy(k):
        nxt = jnp.minimum(st + 1, last)
        return pltpu.make_async_remote_copy(
            src_ref=buf.at[k], dst_ref=buf.at[k + chunks], send_sem=st_send.at[k], recv_sem=st_recv.at[k],
            device_id={'stage': nxt}, device_id_type=MESH)

    def latent_copy(k, dst):
        return pltpu.make_async_remote_copy(
            src_ref=xb.at[k + chunks], dst_ref=xb.at[k + chunks], send_sem=x_send.at[dst, k], recv_sem=x_recv.at[k],
            device_id={'stage': dst}, device_id_type=MESH)

    def xout_copy(c, dst):
        return pltpu.make_async_remote_copy(
            src_ref=xf.at[c], dst_ref=xf.at[c], send_sem=xo_send.at[dst, c], recv_sem=xo_recv.at[c],
            device_id={'stage': dst}, device_id_type=MESH)

    def wait_inputs(k):
        @pl.when(k < chunks)
        def _():
            warm_copy(k).wait()

        @pl.when(jnp.logical_and(k >= chunks, st > 0))
        def _():
            stale_copy(k - chunks).wait_recv()

        @pl.when(jnp.logical_and(k >= chunks, st < last))
        def _():
            latent_copy(k - chunks, 0).wait_recv()

    def send_stage(k):
        @pl.when(jnp.logical_and(k < total - chunks, st < last))
        def _():
            stale_copy(k).start()

    def finish_latent(k):
        step, c = lax.div(k, chunks), lax.rem(k, chunks)

        @pl.when(st == last)
        def _():
            x_new = alpha[step] * xf[c] + beta[step] * ebuf[...]
            xf[c] = x_new

            @pl.when(step < steps - 1)
            def _():
                xb[k + chunks] = x_new.astype(BF16)
                for dst in range(last):
                    latent_copy(k, dst).start()

            @pl.when(step == steps - 1)
            def _():
                for dst in range(last):
                    xout_copy(c, dst).start()

    lane = lax.broadcasted_iota(jnp.int32, (HEAD, 4 * TOK), 1)
    left = lax.rem(lane, 2 * TOK) < TOK
    zero_q = jnp.zeros((HEAD, 2 * TOK), BF16)
    blocks = [slice(r * RB, (r + 1) * RB) for r in range(ROWS // RB)]

    def norm(h, dst, rows, step, scale, shift):
        mean = jnp.sum(h, axis=-1, keepdims=True) * INV_D
        cen = h - mean
        var = jnp.sum(cen * cen, axis=-1, keepdims=True) * INV_D
        put(dst, 0, rows, cen * lax.rsqrt(var + 1e-6) * mods[step, scale:scale + 1, :] + mods[step, shift:shift + 1, :])

    def latent_pieces(k):
        def latent(n):
            h_l[:, n * 256:(n + 1) * 256] = dot(xb[k], wide(wlat, tiles=(2 * n, 2 * n + 1)))
        return [(64, functools.partial(latent, n)) for n in range(4)]

    def norm1_pieces(k):
        step = lax.div(k, chunks)

        def norm1(rows):
            h = jnp.where(st > 0, buf[k, rows, :].astype(F32), 0.0) + h_l[rows, :]
            h_a[rows, :] = h
            norm(h, u_a, rows, step, 1, 0)
        return [(40, functools.partial(norm1, rows)) for rows in blocks]

    def proj_pieces():
        def proj_k(n):
            put(k_s, 2 * n, slice(None), dot(wide(u_a), wide(wk, tiles=(2 * n, 2 * n + 1))))

        def proj_qv(n):
            rows = slice(n * 512, (n + 1) * 512)
            put(qv_s, 0, rows, dot_t(wide(wqvt, rows), wide(u_a)))
        return [(256, functools.partial(proj_k, n)) for n in range(4)] + [(512, functools.partial(proj_qv, n)) for n in range(4)]

    h2 = 2 * TOK

    def attend_pieces():
        groups = [(p, hp) for p in range(ROWS // h2) for hp in range(HEADS // 2)]
        probs = {}

        def scores(g):
            p, hp = groups[g]
            r0, l0 = hp * 2 * HEAD, p * h2
            q0 = qv_s[p, r0:r0 + HEAD, :]
            q1 = qv_s[p, r0 + HEAD:r0 + 2 * HEAD, :]
            rhs = jnp.concatenate([jnp.concatenate([q0, zero_q], axis=1), jnp.concatenate([zero_q, q1], axis=1)], axis=0)
            both = dot(k_s[hp, l0:l0 + h2, :], rhs)
            s = jnp.where(left, both[:TOK], both[TOK:])
            e = jnp.exp2((s - jnp.max(s, axis=0, keepdims=True)) * (HEAD ** -0.5 * LOG2E))
            pr = e * (1.0 / jnp.sum(e, axis=0, keepdims=True))
            probs[g] = (jnp.where(left, pr, 0.0).astype(BF16), jnp.where(left, 0.0, pr).astype(BF16))

        def mix(g):
            p, hp = groups[g]
            r0, l0 = D + hp * 2 * HEAD, p * h2
            p_l, p_r = probs.pop(g)
            rhs = jnp.concatenate([
                jnp.concatenate([p_l[:, :h2], zero_q], axis=1), jnp.concatenate([p_r[:, :h2], zero_q], axis=1),
                jnp.concatenate([zero_q, p_l[:, h2:]], axis=1), jnp.concatenate([zero_q, p_r[:, h2:]], axis=1)], axis=0)
            v = jnp.concatenate([qv_s[p, r0:r0 + HEAD, :], qv_s[p, r0 + HEAD:r0 + 2 * HEAD, :]], axis=1)
            ot = dot(v, rhs)
            ot = jnp.concatenate([ot[:, :h2], ot[:, h2:]], axis=0)
            o_s[hp, l0:l0 + h2, :] = ot.T.astype(BF16)

        pieces = []
        for g in range(len(groups) + 1):
            if g < len(groups):
                pieces.append((75, functools.partial(scores, g)))
            if g > 0:
                pieces.append((75, functools.partial(mix, g - 1)))
        return pieces

    def proj_o_pieces(k):
        step = lax.div(k, chunks)

        def proj_o(n):
            cols = slice(n * 256, (n + 1) * 256)
            h_n[:, cols] = h_a[:, cols] + mods[step, 2:3, cols] * dot(wide(o_s), wide(wo, tiles=(2 * n, 2 * n + 1)))
        return [(256, functools.partial(proj_o, n)) for n in range(4)]

    def norm2_pieces(k):
        step = lax.div(k, chunks)
        return [(40, lambda rows=rows: norm(h_n[rows, :], u_b, rows, step, 4, 3)) for rows in blocks]

    def keep_pieces():
        def keep(rows):
            h_b[rows, :] = h_n[rows, :]
        return [(20, functools.partial(keep, rows)) for rows in blocks]

    def up_pieces():
        def up(n):
            z = dot(wide(u_b), wide(wup, tiles=(2 * n, 2 * n + 1)))
            half = 0.5 * z
            t = jnp.tanh(z * (GC0 + GC1 * (z * z)))
            put(hid, 2 * n, slice(None), half + half * t)
        return [(256, functools.partial(up, n)) for n in range(FF // 256)]

    def down_pieces(k):
        step = lax.div(k, chunks)

        def down(n):
            cols = slice(n * 256, (n + 1) * 256)
            y = dot(wide(hid), wide(wdown, tiles=(2 * n, 2 * n + 1)))
            buf[k, :, cols] = (h_b[:, cols] + mods[step, 5:6, cols] * y).astype(BF16)
        return [(1024, functools.partial(down, n)) for n in range(4)]

    def noise(k):
        ebuf[...] = dot(buf[k], wout[...])

    def run(*lists):
        for pieces in lists:
            for _, piece in pieces:
                piece()

    def norms(second, first):
        out = []
        for n in range(len(blocks)):
            out += second[n:n + 1] + first[n:n + 1]
        return out

    def finish_pieces(k, ahead):
        pieces = proj_o_pieces(k)
        if ahead is None:
            return pieces + norm2_pieces(k)
        return pieces + latent_pieces(ahead) + norms(norm2_pieces(k), norm1_pieces(ahead)) + proj_pieces()

    for ld in ld_q:
        ld.wait()

    @pl.loop(0, D // 128)
    def _(ii):
        sl = pl.ds(pl.multiple_of(ii * 128, 128), 128)
        for part in range(2):
            wqvt[ii, part * D:(part + 1) * D, :] = wtmp[part, sl, :].T

    for ld in ld_s + ld_lat:
        ld.wait()
    for c in range(chunks):
        xb[c] = xf[c].astype(BF16)
    wout[...] = wout_t[...].T
    for step in range(steps):
        for j in range(6):
            row = mods_t[j, step:step + 1, :]
            mods[step, j:j + 1, :] = row + 1.0 if j in (1, 4) else row
    wait_inputs(0)
    run(latent_pieces(0), norm1_pieces(0))
    for ld in ld_k:
        ld.wait()
    run(proj_pieces(), attend_pieces())
    for ld in ld_o:
        ld.wait()
    wait_inputs(1)
    run(finish_pieces(0, 1))
    for ld in ld_up + ld_down:
        ld.wait()

    def body(i, ahead):
        if ahead is not None:
            wait_inputs(ahead)
        noise(jnp.maximum(i - 1, 0))
        merge(attend_pieces() + keep_pieces(), up_pieces())
        merge(finish_pieces(i + 1, ahead), down_pieces(i))
        send_stage(i)

    @pl.loop(0, total - 2)
    def _(i):
        body(i, i + 2)

        @pl.when(i > 0)
        def _():
            finish_latent(i - 1)

    body(total - 2, None)
    finish_latent(total - 3)
    noise(total - 2)
    finish_latent(total - 2)
    run(keep_pieces(), up_pieces(), down_pieces(total - 1))
    noise(total - 1)
    finish_latent(total - 1)

    @pl.when(st < last)
    def _():
        @pl.loop(0, total - chunks)
        def _(k):
            stale_copy(k).wait_send()

        for c in range(chunks):
            xout_copy(c, 0).wait_recv()

    @pl.when(st == last)
    def _():
        @pl.loop(0, total - chunks)
        def _(k):
            for dst in range(last):
                latent_copy(k, dst).wait_send()

        for c in range(chunks):
            for dst in range(last):
                xout_copy(c, dst).wait_send()


def solution(mesh):
    def program(x_init, h_warm, w_lat, w_qkv, w_o, w_up, w_down, w_out, ada_mods, alpha_coef, beta_coef):
        batch, steps = x_init.shape[0], ada_mods.shape[0]
        chunks = batch * TOK // ROWS
        total = steps * chunks
        any_spec = pl.BlockSpec(memory_space=pl.ANY)
        vmem_spec = pl.BlockSpec(memory_space=pltpu.VMEM)
        smem = pl.BlockSpec(memory_space=pltpu.SMEM)
        dma = pltpu.SemaphoreType.DMA
        vb, vf = (lambda *shape: pltpu.VMEM(shape, BF16)), (lambda *shape: pltpu.VMEM(shape, F32))
        flops = 2 * total * ROWS * D * D * 13
        x_out, h_all = pl.pallas_call(
            functools.partial(kernel, steps, chunks),
            out_shape=(pltpu.VMEM((chunks, ROWS, CH), F32), pltpu.VMEM((total, ROWS, D), BF16)),
            in_specs=[any_spec] * 9 + [smem] * 2,
            out_specs=(vmem_spec, vmem_spec),
            scratch_shapes=[
                vb(8, CH, 128), vb(8, D, 128), vb(8, 2 * D, 128), vb(8, D, 128), vb(32, D, 128), vb(8, FF, 128),
                vb(CH, D), vb(D, CH), vb(2, D, D), vf(6, steps, D), vf(steps, 6, D),
                vb(total, ROWS, CH), vf(ROWS, CH),
                vf(ROWS, D), vf(ROWS, D), vf(ROWS, D), vf(ROWS, D),
                vb(8, ROWS, 128), vb(8, ROWS, 128), vb(8, ROWS, 128), vb(2, 2 * D, 128), vb(8, ROWS, 128), vb(32, ROWS, 128),
                dma((2,)), dma((3,)), dma((8,)), dma((8,)), dma((8,)), dma((32,)), dma((8,)),
                dma((chunks,)), dma((total - chunks,)), dma((total - chunks,)),
                dma((STAGES - 1, total - chunks)), dma((total - chunks,)), dma((STAGES - 1, chunks)), dma((chunks,)),
            ],
            compiler_params=pltpu.CompilerParams(
                collective_id=0, has_side_effects=True, vmem_limit_bytes=VMEM_LIMIT),
            cost_estimate=pl.CostEstimate(flops=flops, bytes_accessed=40 << 20, transcendentals=0),
        )(x_init.reshape(chunks, ROWS, CH), h_warm.reshape(STAGES - 1, chunks, ROWS, D),
          w_lat[0], w_qkv[0], w_o.reshape(D, D), w_up[0], w_down[0], w_out.T, ada_mods[:, 0].transpose(1, 0, 2), alpha_coef, beta_coef)
        return x_out.reshape(x_init.shape), h_all[total - chunks:].reshape(1, batch, TOK, D)

    return jax.shard_map(program, mesh=mesh,
                         in_specs=(P('data'), P(None, 'data'), P('stage'), P('stage'), P('stage'), P('stage'), P('stage'), P(), P(None, 'stage'), P(), P()),
                         out_specs=(P('data'), P('stage', 'data')), check_vma=False)
```

```python
import functools

import jax
import jax.numpy as jnp
from jax import lax
from jax.experimental import pallas as pl
from jax.experimental.pallas import tpu as pltpu
from jax.sharding import PartitionSpec as P

F32, BF16 = jnp.float32, jnp.bfloat16
MESH = pl.DeviceIdType.MESH
D, HEADS, HEAD, TOK, CH, FF = 1024, 16, 64, 64, 64, 4096
ROWS = 256
RB = 16
STAGES = 4
INV_D = 1.0 / D
GC0 = 0.7978845608028654
GC1 = GC0 * 0.044715
LOG2E = 1.4426950408889634
VMEM_LIMIT = 45 << 20


def dot(a, b):
    return jnp.dot(a, b, preferred_element_type=F32)


def dot_t(a, b):
    return lax.dot_general(a, b, (((1,), (1,)), ((), ())), preferred_element_type=F32)


def merge(first, second):
    total_a = sum(w for w, _ in first)
    total_b = sum(w for w, _ in second)
    ia = ib = 0
    done_a = done_b = 0.0
    while ia < len(first) or ib < len(second):
        take_a = ib >= len(second) or (ia < len(first) and done_a / total_a <= done_b / total_b)
        if take_a:
            w, piece = first[ia]
            ia, done_a = ia + 1, done_a + w
        else:
            w, piece = second[ib]
            ib, done_b = ib + 1, done_b + w
        piece()


def wide(ref, rows=slice(None), tiles=None):
    tiles = range(ref.shape[0]) if tiles is None else tiles
    return jnp.concatenate([ref[c, rows, :] for c in tiles], axis=1)


def put(ref, first, rows, value):
    for c in range(value.shape[1] // 128):
        ref[first + c, rows, :] = value[:, c * 128:(c + 1) * 128].astype(BF16)


def kernel(steps, chunks,
           x_hbm, warm_hbm, lat_hbm, qkv_hbm, o_hbm, up_hbm, down_hbm, out_hbm, mods_hbm, alpha, beta,
           xf, buf,
           wlat, wk, wqvt, wo, wup, wdown, wout_t, wout, wtmp, mods_t, mods,
           xb, ebuf,
           h_a, h_n, h_b, u_a, u_b, k_s, qv_s, o_s, hid,
           q_sem, s_sem, lat_sem, k_sem, o_sem, up_sem, down_sem,
           warm_sem, st_send, st_recv, x_send, x_recv, xo_send, xo_recv):
    st = lax.axis_index('stage')
    last = STAGES - 1
    total = steps * chunks

    def tiled(src, first, dst, sem):
        return [pltpu.make_async_copy(src.at[:, pl.ds(first + c * 128, 128)], dst.at[c], sem.at[c]) for c in range(dst.shape[0])]

    ld_q = [pltpu.make_async_copy(qkv_hbm.at[:, pl.ds(part * 2 * D, D)], wtmp.at[part], q_sem.at[part]) for part in range(2)]
    ld_s = [pltpu.make_async_copy(src, dst, s_sem.at[n])
            for n, (src, dst) in enumerate(((x_hbm, xf), (mods_hbm, mods_t), (out_hbm, wout_t)))]
    ld_lat = tiled(lat_hbm, 0, wlat, lat_sem)
    ld_k = tiled(qkv_hbm, D, wk, k_sem)
    ld_o = tiled(o_hbm, 0, wo, o_sem)
    ld_up = tiled(up_hbm, 0, wup, up_sem)
    ld_down = tiled(down_hbm, 0, wdown, down_sem)
    warm_stage = jnp.maximum(st - 1, 0)

    def warm_copy(c):
        return pltpu.make_async_copy(warm_hbm.at[warm_stage, c], buf.at[c], warm_sem.at[c])

    for ld in ld_q + ld_s + ld_lat:
        ld.start()
    warm_copy(0).start()
    for ld in ld_k + ld_o:
        ld.start()
    warm_copy(1).start()
    for ld in ld_up + ld_down:
        ld.start()
    for c in range(2, chunks):
        warm_copy(c).start()

    barrier = pltpu.get_barrier_semaphore()
    for k in range(1, STAGES):
        pl.semaphore_signal(barrier, inc=1, device_id={'stage': lax.rem(st + k, STAGES)}, device_id_type=MESH)
    pl.semaphore_wait(barrier, STAGES - 1)

    def stale_copy(k):
        nxt = jnp.minimum(st + 1, last)
        return pltpu.make_async_remote_copy(
            src_ref=buf.at[k], dst_ref=buf.at[k + chunks], send_sem=st_send.at[k], recv_sem=st_recv.at[k],
            device_id={'stage': nxt}, device_id_type=MESH)

    def latent_copy(k, dst):
        return pltpu.make_async_remote_copy(
            src_ref=xb.at[k + chunks], dst_ref=xb.at[k + chunks], send_sem=x_send.at[dst, k], recv_sem=x_recv.at[k],
            device_id={'stage': dst}, device_id_type=MESH)

    def xout_copy(c, dst):
        return pltpu.make_async_remote_copy(
            src_ref=xf.at[c], dst_ref=xf.at[c], send_sem=xo_send.at[dst, c], recv_sem=xo_recv.at[c],
            device_id={'stage': dst}, device_id_type=MESH)

    def wait_inputs(k):
        @pl.when(k < chunks)
        def _():
            warm_copy(k).wait()

        @pl.when(jnp.logical_and(k >= chunks, st > 0))
        def _():
            stale_copy(k - chunks).wait_recv()

        @pl.when(jnp.logical_and(k >= chunks, st < last))
        def _():
            latent_copy(k - chunks, 0).wait_recv()

    def send_stage(k):
        @pl.when(jnp.logical_and(k < total - chunks, st < last))
        def _():
            stale_copy(k).start()

    def finish_latent(k):
        step, c = lax.div(k, chunks), lax.rem(k, chunks)

        @pl.when(st == last)
        def _():
            x_new = alpha[step] * xf[c] + beta[step] * ebuf[...]
            xf[c] = x_new

            @pl.when(step < steps - 1)
            def _():
                xb[k + chunks] = x_new.astype(BF16)
                for dst in range(last):
                    latent_copy(k, dst).start()

            @pl.when(step == steps - 1)
            def _():
                for dst in range(last):
                    xout_copy(c, dst).start()

    lane = lax.broadcasted_iota(jnp.int32, (HEAD, 4 * TOK), 1)
    left = lax.rem(lane, 2 * TOK) < TOK
    zero_q = jnp.zeros((HEAD, 2 * TOK), BF16)
    blocks = [slice(r * RB, (r + 1) * RB) for r in range(ROWS // RB)]

    def norm(h, dst, rows, step, scale, shift):
        mean = jnp.sum(h, axis=-1, keepdims=True) * INV_D
        cen = h - mean
        var = jnp.sum(cen * cen, axis=-1, keepdims=True) * INV_D
        put(dst, 0, rows, cen * lax.rsqrt(var + 1e-6) * mods[step, scale:scale + 1, :] + mods[step, shift:shift + 1, :])

    def latent_pieces(k):
        def latent(n):
            cols = slice(n * 256, (n + 1) * 256)
            stale = jnp.where(st > 0, buf[k, :, cols].astype(F32), 0.0)
            h_a[:, cols] = stale + dot(xb[k], wide(wlat, tiles=(2 * n, 2 * n + 1)))
        return [(64, functools.partial(latent, n)) for n in range(4)]

    def norm1_pieces(k):
        step = lax.div(k, chunks)

        def norm1(rows):
            norm(h_a[rows, :], u_a, rows, step, 1, 0)
        return [(40, functools.partial(norm1, rows)) for rows in blocks]

    def proj_pieces():
        def proj_k(n):
            put(k_s, 2 * n, slice(None), dot(wide(u_a), wide(wk, tiles=(2 * n, 2 * n + 1))))

        def proj_qv(n):
            rows = slice(n * 512, (n + 1) * 512)
            put(qv_s, 0, rows, dot_t(wide(wqvt, rows), wide(u_a)))
        return [(256, functools.partial(proj_k, n)) for n in range(4)] + [(512, functools.partial(proj_qv, n)) for n in range(4)]

    h2 = 2 * TOK

    def attend_pieces():
        groups = [(p, hp) for p in range(ROWS // h2) for hp in range(HEADS // 2)]
        probs = {}

        def scores(g):
            p, hp = groups[g]
            r0, l0 = hp * 2 * HEAD, p * h2
            q0 = qv_s[p, r0:r0 + HEAD, :]
            q1 = qv_s[p, r0 + HEAD:r0 + 2 * HEAD, :]
            rhs = jnp.concatenate([jnp.concatenate([q0, zero_q], axis=1), jnp.concatenate([zero_q, q1], axis=1)], axis=0)
            both = dot(k_s[hp, l0:l0 + h2, :], rhs)
            s = jnp.where(left, both[:TOK], both[TOK:])
            e = jnp.exp2((s - jnp.max(s, axis=0, keepdims=True)) * (HEAD ** -0.5 * LOG2E))
            pr = e * (1.0 / jnp.sum(e, axis=0, keepdims=True))
            probs[g] = (jnp.where(left, pr, 0.0).astype(BF16), jnp.where(left, 0.0, pr).astype(BF16))

        def mix(g):
            p, hp = groups[g]
            r0, l0 = D + hp * 2 * HEAD, p * h2
            p_l, p_r = probs.pop(g)
            rhs = jnp.concatenate([
                jnp.concatenate([p_l[:, :h2], zero_q], axis=1), jnp.concatenate([p_r[:, :h2], zero_q], axis=1),
                jnp.concatenate([zero_q, p_l[:, h2:]], axis=1), jnp.concatenate([zero_q, p_r[:, h2:]], axis=1)], axis=0)
            v = jnp.concatenate([qv_s[p, r0:r0 + HEAD, :], qv_s[p, r0 + HEAD:r0 + 2 * HEAD, :]], axis=1)
            ot = dot(v, rhs)
            ot = jnp.concatenate([ot[:, :h2], ot[:, h2:]], axis=0)
            o_s[hp, l0:l0 + h2, :] = ot.T.astype(BF16)

        pieces = []
        for g in range(len(groups) + 1):
            if g < len(groups):
                pieces.append((75, functools.partial(scores, g)))
            if g > 0:
                pieces.append((75, functools.partial(mix, g - 1)))
        return pieces

    def proj_o_pieces(k):
        step = lax.div(k, chunks)

        def proj_o(n):
            cols = slice(n * 256, (n + 1) * 256)
            h_n[:, cols] = h_a[:, cols] + mods[step, 2:3, cols] * dot(wide(o_s), wide(wo, tiles=(2 * n, 2 * n + 1)))
        return [(256, functools.partial(proj_o, n)) for n in range(4)]

    def norm2_pieces(k):
        step = lax.div(k, chunks)
        return [(40, lambda rows=rows: norm(h_n[rows, :], u_b, rows, step, 4, 3)) for rows in blocks]

    def keep_pieces():
        def keep(rows):
            h_b[rows, :] = h_n[rows, :]
        return [(20, functools.partial(keep, rows)) for rows in blocks]

    def up_pieces():
        def up(n):
            z = dot(wide(u_b), wide(wup, tiles=(2 * n, 2 * n + 1)))
            half = 0.5 * z
            t = jnp.tanh(z * (GC0 + GC1 * (z * z)))
            put(hid, 2 * n, slice(None), half + half * t)
        return [(256, functools.partial(up, n)) for n in range(FF // 256)]

    def down_pieces(k):
        step = lax.div(k, chunks)

        def down(n):
            cols = slice(n * 256, (n + 1) * 256)
            y = dot(wide(hid), wide(wdown, tiles=(2 * n, 2 * n + 1)))
            buf[k, :, cols] = (h_b[:, cols] + mods[step, 5:6, cols] * y).astype(BF16)
        return [(1024, functools.partial(down, n)) for n in range(4)]

    def noise(k):
        ebuf[...] = dot(buf[k], wout[...])

    def run(*lists):
        for pieces in lists:
            for _, piece in pieces:
                piece()

    def norms(second, first):
        out = []
        for n in range(len(blocks)):
            out += second[n:n + 1] + first[n:n + 1]
        return out

    def finish(k, ahead, down):
        run(proj_o_pieces(k))
        if ahead is not None:
            run(latent_pieces(ahead))
        run(down[:2])
        if ahead is None:
            run(norm2_pieces(k), down[2:])
        else:
            run(norms(norm2_pieces(k), norm1_pieces(ahead)))
            merge(proj_pieces(), down[2:]) if down else run(proj_pieces())

    for ld in ld_q:
        ld.wait()

    @pl.loop(0, D // 128)
    def _(ii):
        sl = pl.ds(pl.multiple_of(ii * 128, 128), 128)
        for part in range(2):
            wqvt[ii, part * D:(part + 1) * D, :] = wtmp[part, sl, :].T

    for ld in ld_s + ld_lat:
        ld.wait()
    for c in range(chunks):
        xb[c] = xf[c].astype(BF16)
    wout[...] = wout_t[...].T
    for step in range(steps):
        for j in range(6):
            row = mods_t[step * 6 + j]
            mods[step, j:j + 1, :] = row + 1.0 if j in (1, 4) else row
    wait_inputs(0)
    run(latent_pieces(0), norm1_pieces(0))
    for ld in ld_k:
        ld.wait()
    run(proj_pieces(), attend_pieces())
    for ld in ld_o:
        ld.wait()
    wait_inputs(1)
    finish(0, 1, [])
    for ld in ld_up + ld_down:
        ld.wait()

    def body(i, ahead):
        if ahead is not None:
            wait_inputs(ahead)
        merge(attend_pieces() + keep_pieces(), up_pieces())
        noise(jnp.maximum(i - 1, 0))
        finish(i + 1, ahead, down_pieces(i))
        send_stage(i)

    @pl.loop(0, total - 2)
    def _(i):
        body(i, i + 2)

        @pl.when(i > 0)
        def _():
            finish_latent(i - 1)

    body(total - 2, None)
    finish_latent(total - 3)
    noise(total - 2)
    finish_latent(total - 2)
    run(keep_pieces(), up_pieces(), down_pieces(total - 1))
    noise(total - 1)
    finish_latent(total - 1)

    @pl.when(st < last)
    def _():
        @pl.loop(0, total - chunks)
        def _(k):
            stale_copy(k).wait_send()

        for c in range(chunks):
            xout_copy(c, 0).wait_recv()

    @pl.when(st == last)
    def _():
        @pl.loop(0, total - chunks)
        def _(k):
            for dst in range(last):
                latent_copy(k, dst).wait_send()

        for c in range(chunks):
            for dst in range(last):
                xout_copy(c, dst).wait_send()


def solution(mesh):
    def program(x_init, h_warm, w_lat, w_qkv, w_o, w_up, w_down, w_out, ada_mods, alpha_coef, beta_coef):
        batch, steps = x_init.shape[0], ada_mods.shape[0]
        chunks = batch * TOK // ROWS
        total = steps * chunks
        any_spec = pl.BlockSpec(memory_space=pl.ANY)
        vmem_spec = pl.BlockSpec(memory_space=pltpu.VMEM)
        smem = pl.BlockSpec(memory_space=pltpu.SMEM)
        dma = pltpu.SemaphoreType.DMA
        vb, vf = (lambda *shape: pltpu.VMEM(shape, BF16)), (lambda *shape: pltpu.VMEM(shape, F32))
        flops = 2 * total * ROWS * D * D * 13
        x_out, h_all = pl.pallas_call(
            functools.partial(kernel, steps, chunks),
            out_shape=(pltpu.VMEM((chunks, ROWS, CH), F32), pltpu.VMEM((total, ROWS, D), BF16)),
            in_specs=[any_spec] * 9 + [smem] * 2,
            out_specs=(vmem_spec, vmem_spec),
            scratch_shapes=[
                vb(8, CH, 128), vb(8, D, 128), vb(8, 2 * D, 128), vb(8, D, 128), vb(32, D, 128), vb(8, FF, 128),
                vb(CH, D), vb(D, CH), vb(2, D, D), vf(6 * steps, 1, D), vf(steps, 6, D),
                vb(total, ROWS, CH), vf(ROWS, CH),
                vf(ROWS, D), vf(ROWS, D), vf(ROWS, D),
                vb(8, ROWS, 128), vb(8, ROWS, 128), vb(8, ROWS, 128), vb(2, 2 * D, 128), vb(8, ROWS, 128), vb(32, ROWS, 128),
                dma((2,)), dma((3,)), dma((8,)), dma((8,)), dma((8,)), dma((32,)), dma((8,)),
                dma((chunks,)), dma((total - chunks,)), dma((total - chunks,)),
                dma((STAGES - 1, total - chunks)), dma((total - chunks,)), dma((STAGES - 1, chunks)), dma((chunks,)),
            ],
            compiler_params=pltpu.CompilerParams(
                collective_id=0, has_side_effects=True, vmem_limit_bytes=VMEM_LIMIT),
            cost_estimate=pl.CostEstimate(flops=flops, bytes_accessed=40 << 20, transcendentals=0),
        )(x_init.reshape(chunks, ROWS, CH), h_warm.reshape(STAGES - 1, chunks, ROWS, D),
          w_lat[0], w_qkv[0], w_o.reshape(D, D), w_up[0], w_down[0], w_out.T, ada_mods.reshape(steps * 6, 1, D), alpha_coef, beta_coef)
        return x_out.reshape(x_init.shape), h_all[total - chunks:].reshape(1, batch, TOK, D)

    return jax.shard_map(program, mesh=mesh,
                         in_specs=(P('data'), P(None, 'data'), P('stage'), P('stage'), P('stage'), P('stage'), P('stage'), P(), P(None, 'stage'), P(), P()),
                         out_specs=(P('data'), P('stage', 'data')), check_vma=False)
```

```python
import functools

import jax
import jax.numpy as jnp
from jax import lax
from jax.experimental import pallas as pl
from jax.experimental.pallas import tpu as pltpu
from jax.sharding import PartitionSpec as P

F32, BF16 = jnp.float32, jnp.bfloat16
MESH = pl.DeviceIdType.MESH
D, HEADS, HEAD, TOK, CH, FF = 1024, 16, 64, 64, 64, 4096
ROWS = 256
RB = 16
STAGES = 4
INV_D = 1.0 / D
GC0 = 0.7978845608028654
GC1 = GC0 * 0.044715
LOG2E = 1.4426950408889634
VMEM_LIMIT = 45 << 20


def dot(a, b):
    return jnp.dot(a, b, preferred_element_type=F32)


def merge(first, second):
    total_a = sum(w for w, _ in first)
    total_b = sum(w for w, _ in second)
    ia = ib = 0
    done_a = done_b = 0.0
    while ia < len(first) or ib < len(second):
        take_a = ib >= len(second) or (ia < len(first) and done_a / total_a <= done_b / total_b)
        if take_a:
            w, piece = first[ia]
            ia, done_a = ia + 1, done_a + w
        else:
            w, piece = second[ib]
            ib, done_b = ib + 1, done_b + w
        piece()


def wide(ref, rows=slice(None), tiles=None):
    tiles = range(ref.shape[0]) if tiles is None else tiles
    return jnp.concatenate([ref[c, rows, :] for c in tiles], axis=1)


def put(ref, first, rows, value):
    for c in range(value.shape[1] // 128):
        ref[first + c, rows, :] = value[:, c * 128:(c + 1) * 128].astype(BF16)


def kernel(steps, chunks,
           x_hbm, warm_hbm, lat_hbm, qkv_hbm, o_hbm, up_hbm, down_hbm, out_hbm, mods_hbm, alpha, beta,
           xf, buf,
           wlat, wq, wk, wv, wo, wup, wdown, wout_t, wout, mods_t, mods,
           xb, ebuf,
           h_a, h_n, h_b, u_a, u_b, k_s, qv_s, o_s, hid,
           s_sem, lat_sem, q_sem, k_sem, v_sem, o_sem, up_sem, down_sem,
           warm_sem, st_send, st_recv, x_send, x_recv, xo_send, xo_recv):
    st = lax.axis_index('stage')
    last = STAGES - 1
    total = steps * chunks

    def tiled(src, first, dst, sem):
        return [pltpu.make_async_copy(src.at[:, pl.ds(first + c * 128, 128)], dst.at[c], sem.at[c]) for c in range(dst.shape[0])]

    ld_s = [pltpu.make_async_copy(src, dst, s_sem.at[n])
            for n, (src, dst) in enumerate(((x_hbm, xf), (mods_hbm, mods_t), (out_hbm, wout_t)))]
    ld_lat = tiled(lat_hbm, 0, wlat, lat_sem)
    ld_qkv = tiled(qkv_hbm, 0, wq, q_sem) + tiled(qkv_hbm, D, wk, k_sem) + tiled(qkv_hbm, 2 * D, wv, v_sem)
    ld_o = tiled(o_hbm, 0, wo, o_sem)
    ld_up = tiled(up_hbm, 0, wup, up_sem)
    ld_down = tiled(down_hbm, 0, wdown, down_sem)
    warm_stage = jnp.maximum(st - 1, 0)

    def warm_copy(c):
        return pltpu.make_async_copy(warm_hbm.at[warm_stage, c], buf.at[c], warm_sem.at[c])

    for ld in ld_s + ld_lat:
        ld.start()
    warm_copy(0).start()
    for ld in ld_qkv + ld_o:
        ld.start()
    warm_copy(1).start()

    barrier = pltpu.get_barrier_semaphore()
    for k in range(1, STAGES):
        pl.semaphore_signal(barrier, inc=1, device_id={'stage': lax.rem(st + k, STAGES)}, device_id_type=MESH)

    def stale_copy(k):
        nxt = jnp.minimum(st + 1, last)
        return pltpu.make_async_remote_copy(
            src_ref=buf.at[k], dst_ref=buf.at[k + chunks], send_sem=st_send.at[k], recv_sem=st_recv.at[k],
            device_id={'stage': nxt}, device_id_type=MESH)

    def latent_copy(k, dst):
        return pltpu.make_async_remote_copy(
            src_ref=xb.at[k + chunks], dst_ref=xb.at[k + chunks], send_sem=x_send.at[dst, k], recv_sem=x_recv.at[k],
            device_id={'stage': dst}, device_id_type=MESH)

    def xout_copy(c, dst):
        return pltpu.make_async_remote_copy(
            src_ref=xf.at[c], dst_ref=xf.at[c], send_sem=xo_send.at[dst, c], recv_sem=xo_recv.at[c],
            device_id={'stage': dst}, device_id_type=MESH)

    def wait_inputs(k):
        @pl.when(k < chunks)
        def _():
            warm_copy(k).wait()

        @pl.when(jnp.logical_and(k >= chunks, st > 0))
        def _():
            stale_copy(k - chunks).wait_recv()

        @pl.when(jnp.logical_and(k >= chunks, st < last))
        def _():
            latent_copy(k - chunks, 0).wait_recv()

    def send_stage(k):
        @pl.when(jnp.logical_and(k < total - chunks, st < last))
        def _():
            stale_copy(k).start()

    def finish_latent(k):
        step, c = lax.div(k, chunks), lax.rem(k, chunks)

        @pl.when(st == last)
        def _():
            x_new = alpha[step] * xf[c] + beta[step] * ebuf[...]
            xf[c] = x_new

            @pl.when(step < steps - 1)
            def _():
                xb[k + chunks] = x_new.astype(BF16)
                for dst in range(last):
                    latent_copy(k, dst).start()

            @pl.when(step == steps - 1)
            def _():
                for dst in range(last):
                    xout_copy(c, dst).start()

    lane = lax.broadcasted_iota(jnp.int32, (HEAD, 4 * TOK), 1)
    left = lax.rem(lane, 2 * TOK) < TOK
    zero_q = jnp.zeros((HEAD, 2 * TOK), BF16)
    blocks = [slice(r * RB, (r + 1) * RB) for r in range(ROWS // RB)]

    def norm(h, dst, rows, step, scale, shift):
        mean = jnp.sum(h, axis=-1, keepdims=True) * INV_D
        cen = h - mean
        var = jnp.sum(cen * cen, axis=-1, keepdims=True) * INV_D
        put(dst, 0, rows, cen * lax.rsqrt(var + 1e-6) * mods[step, scale:scale + 1, :] + mods[step, shift:shift + 1, :])

    def latent_pieces(k):
        def latent(n):
            cols = slice(n * 256, (n + 1) * 256)
            stale = jnp.where(st > 0, buf[k, :, cols].astype(F32), 0.0)
            h_a[:, cols] = stale + dot(xb[k], wide(wlat, tiles=(2 * n, 2 * n + 1)))
        return [(64, functools.partial(latent, n)) for n in range(4)]

    def norm1_pieces(k):
        step = lax.div(k, chunks)

        def norm1(rows):
            norm(h_a[rows, :], u_a, rows, step, 1, 0)
        return [(40, functools.partial(norm1, rows)) for rows in blocks]

    def proj_pieces():
        def proj_k(n):
            put(k_s, 2 * n, slice(None), dot(wide(u_a), wide(wk, tiles=(2 * n, 2 * n + 1))))

        def proj_qv(n):
            part, w = (0, wq) if n < 4 else (D, wv)
            n = n % 4
            val = dot(wide(u_a), wide(w, tiles=(2 * n, 2 * n + 1))).astype(BF16).T
            put(qv_s, 0, slice(part + n * 256, part + (n + 1) * 256), val)
        return [(256, functools.partial(proj_qv, n)) for n in range(8)] + [(256, functools.partial(proj_k, n)) for n in range(4)]

    h2 = 2 * TOK

    def attend_pieces():
        groups = [(p, hp) for p in range(ROWS // h2) for hp in range(HEADS // 2)]
        probs = {}

        def scores(g):
            p, hp = groups[g]
            r0, l0 = hp * 2 * HEAD, p * h2
            q0 = qv_s[p, r0:r0 + HEAD, :]
            q1 = qv_s[p, r0 + HEAD:r0 + 2 * HEAD, :]
            rhs = jnp.concatenate([jnp.concatenate([q0, zero_q], axis=1), jnp.concatenate([zero_q, q1], axis=1)], axis=0)
            both = dot(k_s[hp, l0:l0 + h2, :], rhs)
            s = jnp.where(left, both[:TOK], both[TOK:])
            e = jnp.exp2((s - jnp.max(s, axis=0, keepdims=True)) * (HEAD ** -0.5 * LOG2E))
            pr = e * (1.0 / jnp.sum(e, axis=0, keepdims=True))
            probs[g] = (jnp.where(left, pr, 0.0).astype(BF16), jnp.where(left, 0.0, pr).astype(BF16))

        def mix(g):
            p, hp = groups[g]
            r0, l0 = D + hp * 2 * HEAD, p * h2
            p_l, p_r = probs.pop(g)
            rhs = jnp.concatenate([
                jnp.concatenate([p_l[:, :h2], zero_q], axis=1), jnp.concatenate([p_r[:, :h2], zero_q], axis=1),
                jnp.concatenate([zero_q, p_l[:, h2:]], axis=1), jnp.concatenate([zero_q, p_r[:, h2:]], axis=1)], axis=0)
            v = jnp.concatenate([qv_s[p, r0:r0 + HEAD, :], qv_s[p, r0 + HEAD:r0 + 2 * HEAD, :]], axis=1)
            ot = dot(v, rhs)
            ot = jnp.concatenate([ot[:, :h2], ot[:, h2:]], axis=0)
            o_s[hp, l0:l0 + h2, :] = ot.astype(BF16).T

        pieces = []
        for g in range(len(groups) + 1):
            if g < len(groups):
                pieces.append((75, functools.partial(scores, g)))
            if g > 0:
                pieces.append((75, functools.partial(mix, g - 1)))
        return pieces

    def proj_o_pieces(k):
        step = lax.div(k, chunks)

        def proj_o(n):
            cols = slice(n * 256, (n + 1) * 256)
            h_n[:, cols] = h_a[:, cols] + mods[step, 2:3, cols] * dot(wide(o_s), wide(wo, tiles=(2 * n, 2 * n + 1)))
        return [(256, functools.partial(proj_o, n)) for n in range(4)]

    def norm2_pieces(k):
        step = lax.div(k, chunks)
        return [(40, lambda rows=rows: norm(h_n[rows, :], u_b, rows, step, 4, 3)) for rows in blocks]

    def keep_pieces():
        def keep(rows):
            h_b[rows, :] = h_n[rows, :]
        return [(20, functools.partial(keep, rows)) for rows in blocks]

    def up_pieces():
        def up(n):
            z = dot(wide(u_b), wide(wup, tiles=(2 * n, 2 * n + 1)))
            half = 0.5 * z
            t = jnp.tanh(z * (GC0 + GC1 * (z * z)))
            put(hid, 2 * n, slice(None), half + half * t)
        return [(256, functools.partial(up, n)) for n in range(FF // 256)]

    def down_pieces(k):
        step = lax.div(k, chunks)

        def down(n):
            cols = slice(n * 256, (n + 1) * 256)
            y = dot(wide(hid), wide(wdown, tiles=(2 * n, 2 * n + 1)))
            buf[k, :, cols] = (h_b[:, cols] + mods[step, 5:6, cols] * y).astype(BF16)
        return [(1024, functools.partial(down, n)) for n in range(4)]

    def noise(k):
        ebuf[...] = dot(buf[k], wout[...])

    def run(*lists):
        for pieces in lists:
            for _, piece in pieces:
                piece()

    def norms(second, first):
        out = []
        for n in range(len(blocks)):
            out += second[n:n + 1] + first[n:n + 1]
        return out

    def finish(k, ahead, down):
        run(proj_o_pieces(k))
        if ahead is not None:
            run(latent_pieces(ahead))
        run(down[:2])
        if ahead is None:
            run(norm2_pieces(k), down[2:])
        else:
            run(norms(norm2_pieces(k), norm1_pieces(ahead)))
            merge(proj_pieces(), down[2:]) if down else run(proj_pieces())

    for ld in ld_s + ld_lat:
        ld.wait()
    for c in range(chunks):
        xb[c] = xf[c].astype(BF16)
    wout[...] = wout_t[...].T
    for step in range(steps):
        for j in range(6):
            row = mods_t[step * 6 + j]
            mods[step, j:j + 1, :] = row + 1.0 if j in (1, 4) else row
    wait_inputs(0)
    run(latent_pieces(0), norm1_pieces(0))
    for ld in ld_qkv:
        ld.wait()
    for ld in ld_up + ld_down:
        ld.start()
    for c in range(2, chunks):
        warm_copy(c).start()
    run(proj_pieces(), attend_pieces())
    for ld in ld_o:
        ld.wait()
    wait_inputs(1)
    finish(0, 1, [])
    for ld in ld_up + ld_down:
        ld.wait()
    pl.semaphore_wait(barrier, STAGES - 1)

    def body(i, ahead):
        if ahead is not None:
            wait_inputs(ahead)
        merge(attend_pieces() + keep_pieces(), up_pieces())
        noise(jnp.maximum(i - 1, 0))
        finish(i + 1, ahead, down_pieces(i))
        send_stage(i)

    @pl.loop(0, total - 2)
    def _(i):
        body(i, i + 2)

        @pl.when(i > 0)
        def _():
            finish_latent(i - 1)

    body(total - 2, None)
    finish_latent(total - 3)
    noise(total - 2)
    finish_latent(total - 2)
    run(keep_pieces(), up_pieces(), down_pieces(total - 1))
    noise(total - 1)
    finish_latent(total - 1)

    @pl.when(st < last)
    def _():
        @pl.loop(0, total - chunks)
        def _(k):
            stale_copy(k).wait_send()

        for c in range(chunks):
            xout_copy(c, 0).wait_recv()

    @pl.when(st == last)
    def _():
        @pl.loop(0, total - chunks)
        def _(k):
            for dst in range(last):
                latent_copy(k, dst).wait_send()

        for c in range(chunks):
            for dst in range(last):
                xout_copy(c, dst).wait_send()


def solution(mesh):
    def program(x_init, h_warm, w_lat, w_qkv, w_o, w_up, w_down, w_out, ada_mods, alpha_coef, beta_coef):
        batch, steps = x_init.shape[0], ada_mods.shape[0]
        chunks = batch * TOK // ROWS
        total = steps * chunks
        any_spec = pl.BlockSpec(memory_space=pl.ANY)
        vmem_spec = pl.BlockSpec(memory_space=pltpu.VMEM)
        smem = pl.BlockSpec(memory_space=pltpu.SMEM)
        dma = pltpu.SemaphoreType.DMA
        vb, vf = (lambda *shape: pltpu.VMEM(shape, BF16)), (lambda *shape: pltpu.VMEM(shape, F32))
        flops = 2 * total * ROWS * D * D * 13
        x_out, h_all = pl.pallas_call(
            functools.partial(kernel, steps, chunks),
            out_shape=(pltpu.VMEM((chunks, ROWS, CH), F32), pltpu.VMEM((total, ROWS, D), BF16)),
            in_specs=[any_spec] * 9 + [smem] * 2,
            out_specs=(vmem_spec, vmem_spec),
            scratch_shapes=[
                vb(8, CH, 128), vb(8, D, 128), vb(8, D, 128), vb(8, D, 128), vb(8, D, 128), vb(32, D, 128), vb(8, FF, 128),
                vb(CH, D), vb(D, CH), vf(6 * steps, 1, D), vf(steps, 6, D),
                vb(total, ROWS, CH), vf(ROWS, CH),
                vf(ROWS, D), vf(ROWS, D), vf(ROWS, D),
                vb(8, ROWS, 128), vb(8, ROWS, 128), vb(8, ROWS, 128), vb(2, 2 * D, 128), vb(8, ROWS, 128), vb(32, ROWS, 128),
                dma((3,)), dma((8,)), dma((8,)), dma((8,)), dma((8,)), dma((8,)), dma((32,)), dma((8,)),
                dma((chunks,)), dma((total - chunks,)), dma((total - chunks,)),
                dma((STAGES - 1, total - chunks)), dma((total - chunks,)), dma((STAGES - 1, chunks)), dma((chunks,)),
            ],
            compiler_params=pltpu.CompilerParams(
                collective_id=0, has_side_effects=True, vmem_limit_bytes=VMEM_LIMIT),
            cost_estimate=pl.CostEstimate(flops=flops, bytes_accessed=40 << 20, transcendentals=0),
        )(x_init.reshape(chunks, ROWS, CH), h_warm.reshape(STAGES - 1, chunks, ROWS, D),
          w_lat[0], w_qkv[0], w_o.reshape(D, D), w_up[0], w_down[0], w_out.T, ada_mods.reshape(steps * 6, 1, D), alpha_coef, beta_coef)
        return x_out.reshape(x_init.shape), h_all[total - chunks:].reshape(1, batch, TOK, D)

    return jax.shard_map(program, mesh=mesh,
                         in_specs=(P('data'), P(None, 'data'), P('stage'), P('stage'), P('stage'), P('stage'), P('stage'), P(), P(None, 'stage'), P(), P()),
                         out_specs=(P('data'), P('stage', 'data')), check_vma=False)
```

```python
import functools

import jax
import jax.numpy as jnp
from jax import lax
from jax.experimental import pallas as pl
from jax.experimental.pallas import tpu as pltpu
from jax.sharding import PartitionSpec as P

F32, BF16 = jnp.float32, jnp.bfloat16
MESH = pl.DeviceIdType.MESH
D, HEADS, HEAD, TOK, CH, FF = 1024, 16, 64, 64, 64, 4096
ROWS = 256
RB = 16
STAGES = 4
INV_D = 1.0 / D
GC0 = 0.7978845608028654
GC1 = GC0 * 0.044715
LOG2E = 1.4426950408889634
TRAIL, LAG, LEAD = 3, 4, 3
VMEM_LIMIT = 45 << 20


def dot(a, b):
    return jnp.dot(a, b, preferred_element_type=F32)


def merge(first, second):
    total_a = sum(w for w, _ in first)
    total_b = sum(w for w, _ in second)
    ia = ib = 0
    done_a = done_b = 0.0
    while ia < len(first) or ib < len(second):
        take_a = ib >= len(second) or (ia < len(first) and done_a / total_a <= done_b / total_b)
        if take_a:
            w, piece = first[ia]
            ia, done_a = ia + 1, done_a + w
        else:
            w, piece = second[ib]
            ib, done_b = ib + 1, done_b + w
        piece()


def wide(ref, rows=slice(None), tiles=None):
    tiles = range(ref.shape[0]) if tiles is None else tiles
    return jnp.concatenate([ref[c, rows, :] for c in tiles], axis=1)


def put(ref, first, rows, value):
    for c in range(value.shape[1] // 128):
        ref[first + c, rows, :] = value[:, c * 128:(c + 1) * 128].astype(BF16)


def kernel(steps, chunks,
           x_hbm, warm_hbm, lat_hbm, qkv_hbm, o_hbm, up_hbm, down_hbm, out_hbm, mods_hbm, alpha, beta,
           xf, buf,
           wlat, wq, wk, wv, wo, wup, wdown, wout_t, wout, mods_t, mods,
           xb, ebuf,
           h_a, h_n, h_b, u_a, u_b, k_s, qv_s, p_s, o_s, hid,
           s_sem, lat_sem, q_sem, k_sem, v_sem, o_sem, up_sem, down_sem,
           warm_sem, st_send, st_recv, x_send, x_recv, xo_send, xo_recv):
    st = lax.axis_index('stage')
    last = STAGES - 1
    total = steps * chunks

    def tiled(src, first, dst, sem):
        return [pltpu.make_async_copy(src.at[:, pl.ds(first + c * 128, 128)], dst.at[c], sem.at[c]) for c in range(dst.shape[0])]

    ld_s = [pltpu.make_async_copy(src, dst, s_sem.at[n])
            for n, (src, dst) in enumerate(((x_hbm, xf), (mods_hbm, mods_t), (out_hbm, wout_t)))]
    ld_lat = tiled(lat_hbm, 0, wlat, lat_sem)
    ld_qkv = tiled(qkv_hbm, 0, wq, q_sem) + tiled(qkv_hbm, D, wk, k_sem) + tiled(qkv_hbm, 2 * D, wv, v_sem)
    ld_o = tiled(o_hbm, 0, wo, o_sem)
    ld_up = tiled(up_hbm, 0, wup, up_sem)
    ld_down = tiled(down_hbm, 0, wdown, down_sem)
    warm_stage = jnp.maximum(st - 1, 0)

    def warm_copy(c):
        return pltpu.make_async_copy(warm_hbm.at[warm_stage, c], buf.at[c], warm_sem.at[c])

    for ld in ld_s + ld_lat:
        ld.start()
    warm_copy(0).start()
    for ld in ld_qkv + ld_o:
        ld.start()
    warm_copy(1).start()

    barrier = pltpu.get_barrier_semaphore()
    for k in range(1, STAGES):
        pl.semaphore_signal(barrier, inc=1, device_id={'stage': lax.rem(st + k, STAGES)}, device_id_type=MESH)

    def stale_copy(k):
        nxt = jnp.minimum(st + 1, last)
        return pltpu.make_async_remote_copy(
            src_ref=buf.at[k], dst_ref=buf.at[k + chunks], send_sem=st_send.at[k], recv_sem=st_recv.at[k],
            device_id={'stage': nxt}, device_id_type=MESH)

    def latent_copy(k, dst):
        return pltpu.make_async_remote_copy(
            src_ref=xb.at[k + chunks], dst_ref=xb.at[k + chunks], send_sem=x_send.at[dst, k], recv_sem=x_recv.at[k],
            device_id={'stage': dst}, device_id_type=MESH)

    def xout_copy(c, dst):
        return pltpu.make_async_remote_copy(
            src_ref=xf.at[c], dst_ref=xf.at[c], send_sem=xo_send.at[dst, c], recv_sem=xo_recv.at[c],
            device_id={'stage': dst}, device_id_type=MESH)

    def wait_inputs(k):
        @pl.when(k < chunks)
        def _():
            warm_copy(k).wait()

        @pl.when(jnp.logical_and(k >= chunks, st > 0))
        def _():
            stale_copy(k - chunks).wait_recv()

        @pl.when(jnp.logical_and(k >= chunks, st < last))
        def _():
            latent_copy(k - chunks, 0).wait_recv()

    def send_stage(k):
        @pl.when(jnp.logical_and(k < total - chunks, st < last))
        def _():
            stale_copy(k).start()

    def finish_latent(k):
        step, c = lax.div(k, chunks), lax.rem(k, chunks)

        @pl.when(st == last)
        def _():
            x_new = alpha[step] * xf[c] + beta[step] * ebuf[...]
            xf[c] = x_new

            @pl.when(step < steps - 1)
            def _():
                xb[k + chunks] = x_new.astype(BF16)
                for dst in range(last):
                    latent_copy(k, dst).start()

            @pl.when(step == steps - 1)
            def _():
                for dst in range(last):
                    xout_copy(c, dst).start()

    lane = lax.broadcasted_iota(jnp.int32, (HEAD, 4 * TOK), 1)
    left = lax.rem(lane, 2 * TOK) < TOK
    zero_q = jnp.zeros((HEAD, 2 * TOK), BF16)
    blocks = [slice(r * RB, (r + 1) * RB) for r in range(ROWS // RB)]

    def norm(h, dst, rows, step, scale, shift):
        mean = jnp.sum(h, axis=-1, keepdims=True) * INV_D
        cen = h - mean
        var = jnp.sum(cen * cen, axis=-1, keepdims=True) * INV_D
        put(dst, 0, rows, cen * lax.rsqrt(var + 1e-6) * mods[step, scale:scale + 1, :] + mods[step, shift:shift + 1, :])

    def latent_pieces(k):
        def latent(n):
            cols = slice(n * 256, (n + 1) * 256)
            stale = jnp.where(st > 0, buf[k, :, cols].astype(F32), 0.0)
            h_a[:, cols] = stale + dot(xb[k], wide(wlat, tiles=(2 * n, 2 * n + 1)))
        return [(64, functools.partial(latent, n)) for n in range(4)]

    def norm1_pieces(k):
        step = lax.div(k, chunks)

        def norm1(rows):
            norm(h_a[rows, :], u_a, rows, step, 1, 0)
        return [(40, functools.partial(norm1, rows)) for rows in blocks]

    def proj_pieces():
        def proj_k(n):
            put(k_s, 2 * n, slice(None), dot(wide(u_a), wide(wk, tiles=(2 * n, 2 * n + 1))))

        def proj_qv(n):
            part, w = (0, wq) if n < 4 else (D, wv)
            n = n % 4
            val = dot(wide(u_a), wide(w, tiles=(2 * n, 2 * n + 1))).astype(BF16).T
            put(qv_s, 0, slice(part + n * 256, part + (n + 1) * 256), val)
        return [(256, functools.partial(proj_qv, n)) for n in range(8)] + [(256, functools.partial(proj_k, n)) for n in range(4)]

    h2 = 2 * TOK

    def attend_pieces():
        groups = [(p, hp) for p in range(ROWS // h2) for hp in range(HEADS // 2)]

        def scores(g):
            p, hp = groups[g]
            r0, l0 = hp * 2 * HEAD, p * h2
            q0 = qv_s[p, r0:r0 + HEAD, :]
            q1 = qv_s[p, r0 + HEAD:r0 + 2 * HEAD, :]
            rhs = jnp.concatenate([jnp.concatenate([q0, zero_q], axis=1), jnp.concatenate([zero_q, q1], axis=1)], axis=0)
            both = dot(k_s[hp, l0:l0 + h2, :], rhs)
            s = jnp.where(left, both[:TOK], both[TOK:])
            e = jnp.exp2((s - jnp.max(s, axis=0, keepdims=True)) * (HEAD ** -0.5 * LOG2E))
            pr = e * (1.0 / jnp.sum(e, axis=0, keepdims=True))
            put(p_s, 4 * g, slice(None), jnp.where(left, pr, 0.0))
            put(p_s, 4 * g + 2, slice(None), jnp.where(left, 0.0, pr))

        def mix(g):
            p, hp = groups[g]
            r0, l0 = D + hp * 2 * HEAD, p * h2
            rhs = jnp.concatenate([
                jnp.concatenate([p_s[4 * g], zero_q], axis=1), jnp.concatenate([p_s[4 * g + 2], zero_q], axis=1),
                jnp.concatenate([zero_q, p_s[4 * g + 1]], axis=1), jnp.concatenate([zero_q, p_s[4 * g + 3]], axis=1)], axis=0)
            v = jnp.concatenate([qv_s[p, r0:r0 + HEAD, :], qv_s[p, r0 + HEAD:r0 + 2 * HEAD, :]], axis=1)
            ot = dot(v, rhs)
            ot = jnp.concatenate([ot[:, :h2], ot[:, h2:]], axis=0)
            o_s[hp, l0:l0 + h2, :] = ot.astype(BF16).T

        return ([functools.partial(scores, g) for g in range(len(groups))],
                [functools.partial(mix, g) for g in range(len(groups))])

    def attend_up():
        scores, mixes = attend_pieces()
        keeps, ups = keep_pieces(), up_pieces()
        done_s = done_m = 0
        for n, (_, up) in enumerate(ups):
            up()
            keeps[n][1]()
            while done_s < min(len(scores), (n + 1) * len(scores) / (len(ups) - TRAIL)):
                scores[done_s]()
                done_s += 1
            while done_m < min(len(mixes), done_s - LAG if n < len(ups) - TRAIL else (n + 1 - LEAD) * len(mixes) / (len(ups) - LEAD)):
                mixes[done_m]()
                done_m += 1

    def proj_o_pieces(k):
        step = lax.div(k, chunks)

        def proj_o(n):
            cols = slice(n * 256, (n + 1) * 256)
            h_n[:, cols] = h_a[:, cols] + mods[step, 2:3, cols] * dot(wide(o_s), wide(wo, tiles=(2 * n, 2 * n + 1)))
        return [(256, functools.partial(proj_o, n)) for n in range(4)]

    def norm2_pieces(k):
        step = lax.div(k, chunks)
        return [(40, lambda rows=rows: norm(h_n[rows, :], u_b, rows, step, 4, 3)) for rows in blocks]

    def keep_pieces():
        def keep(rows):
            h_b[rows, :] = h_n[rows, :]
        return [(20, functools.partial(keep, rows)) for rows in blocks]

    def up_pieces():
        def up(n):
            z = dot(wide(u_b), wide(wup, tiles=(2 * n, 2 * n + 1)))
            half = 0.5 * z
            t = jnp.tanh(z * (GC0 + GC1 * (z * z)))
            put(hid, 2 * n, slice(None), half + half * t)
        return [(256, functools.partial(up, n)) for n in range(FF // 256)]

    def down_pieces(k):
        step = lax.div(k, chunks)

        def down(n):
            cols = slice(n * 256, (n + 1) * 256)
            y = dot(wide(hid), wide(wdown, tiles=(2 * n, 2 * n + 1)))
            buf[k, :, cols] = (h_b[:, cols] + mods[step, 5:6, cols] * y).astype(BF16)
        return [(1024, functools.partial(down, n)) for n in range(4)]

    def noise(k):
        ebuf[...] = dot(buf[k], wout[...])

    def run(*lists):
        for pieces in lists:
            for _, piece in pieces:
                piece()

    def norms(second, first):
        out = []
        for n in range(len(blocks)):
            out += second[n:n + 1] + first[n:n + 1]
        return out

    def finish(k, ahead, down):
        run(proj_o_pieces(k))
        if ahead is not None:
            run(latent_pieces(ahead))
        run(down[:2])
        if ahead is None:
            run(norm2_pieces(k), down[2:])
        else:
            run(norms(norm2_pieces(k), norm1_pieces(ahead)))
            merge(proj_pieces(), down[2:]) if down else run(proj_pieces())

    for ld in ld_s + ld_lat:
        ld.wait()
    for c in range(chunks):
        xb[c] = xf[c].astype(BF16)
    wout[...] = wout_t[...].T
    for step in range(steps):
        for j in range(6):
            row = mods_t[step * 6 + j]
            mods[step, j:j + 1, :] = row + 1.0 if j in (1, 4) else row
    wait_inputs(0)
    run(latent_pieces(0), norm1_pieces(0))
    for ld in ld_qkv:
        ld.wait()
    for ld in ld_up + ld_down:
        ld.start()
    for c in range(2, chunks):
        warm_copy(c).start()
    run(proj_pieces())
    for pieces in attend_pieces():
        for piece in pieces:
            piece()
    for ld in ld_o:
        ld.wait()
    wait_inputs(1)
    finish(0, 1, [])
    for ld in ld_up + ld_down:
        ld.wait()
    pl.semaphore_wait(barrier, STAGES - 1)

    def body(i, ahead):
        if ahead is not None:
            wait_inputs(ahead)
        attend_up()
        noise(jnp.maximum(i - 1, 0))
        finish(i + 1, ahead, down_pieces(i))
        send_stage(i)

    @pl.loop(0, total - 2)
    def _(i):
        body(i, i + 2)

        @pl.when(i > 0)
        def _():
            finish_latent(i - 1)

    body(total - 2, None)
    finish_latent(total - 3)
    noise(total - 2)
    finish_latent(total - 2)
    run(keep_pieces(), up_pieces(), down_pieces(total - 1))
    noise(total - 1)
    finish_latent(total - 1)

    @pl.when(st < last)
    def _():
        @pl.loop(0, total - chunks)
        def _(k):
            stale_copy(k).wait_send()

        for c in range(chunks):
            xout_copy(c, 0).wait_recv()

    @pl.when(st == last)
    def _():
        @pl.loop(0, total - chunks)
        def _(k):
            for dst in range(last):
                latent_copy(k, dst).wait_send()

        for c in range(chunks):
            for dst in range(last):
                xout_copy(c, dst).wait_send()


def solution(mesh):
    def program(x_init, h_warm, w_lat, w_qkv, w_o, w_up, w_down, w_out, ada_mods, alpha_coef, beta_coef):
        batch, steps = x_init.shape[0], ada_mods.shape[0]
        chunks = batch * TOK // ROWS
        total = steps * chunks
        any_spec = pl.BlockSpec(memory_space=pl.ANY)
        vmem_spec = pl.BlockSpec(memory_space=pltpu.VMEM)
        smem = pl.BlockSpec(memory_space=pltpu.SMEM)
        dma = pltpu.SemaphoreType.DMA
        vb, vf = (lambda *shape: pltpu.VMEM(shape, BF16)), (lambda *shape: pltpu.VMEM(shape, F32))
        flops = 2 * total * ROWS * D * D * 13
        x_out, h_all = pl.pallas_call(
            functools.partial(kernel, steps, chunks),
            out_shape=(pltpu.VMEM((chunks, ROWS, CH), F32), pltpu.VMEM((total, ROWS, D), BF16)),
            in_specs=[any_spec] * 9 + [smem] * 2,
            out_specs=(vmem_spec, vmem_spec),
            scratch_shapes=[
                vb(8, CH, 128), vb(8, D, 128), vb(8, D, 128), vb(8, D, 128), vb(8, D, 128), vb(32, D, 128), vb(8, FF, 128),
                vb(CH, D), vb(D, CH), vf(6 * steps, 1, D), vf(steps, 6, D),
                vb(total, ROWS, CH), vf(ROWS, CH),
                vf(ROWS, D), vf(ROWS, D), vf(ROWS, D),
                vb(8, ROWS, 128), vb(8, ROWS, 128), vb(8, ROWS, 128), vb(2, 2 * D, 128), vb(64, TOK, 128), vb(8, ROWS, 128), vb(32, ROWS, 128),
                dma((3,)), dma((8,)), dma((8,)), dma((8,)), dma((8,)), dma((8,)), dma((32,)), dma((8,)),
                dma((chunks,)), dma((total - chunks,)), dma((total - chunks,)),
                dma((STAGES - 1, total - chunks)), dma((total - chunks,)), dma((STAGES - 1, chunks)), dma((chunks,)),
            ],
            compiler_params=pltpu.CompilerParams(
                collective_id=0, has_side_effects=True, vmem_limit_bytes=VMEM_LIMIT),
            cost_estimate=pl.CostEstimate(flops=flops, bytes_accessed=40 << 20, transcendentals=0),
        )(x_init.reshape(chunks, ROWS, CH), h_warm.reshape(STAGES - 1, chunks, ROWS, D),
          w_lat[0], w_qkv[0], w_o.reshape(D, D), w_up[0], w_down[0], w_out.T, ada_mods.reshape(steps * 6, 1, D), alpha_coef, beta_coef)
        return x_out.reshape(x_init.shape), h_all[total - chunks:].reshape(1, batch, TOK, D)

    return jax.shard_map(program, mesh=mesh,
                         in_specs=(P('data'), P(None, 'data'), P('stage'), P('stage'), P('stage'), P('stage'), P('stage'), P(), P(None, 'stage'), P(), P()),
                         out_specs=(P('data'), P('stage', 'data')), check_vma=False)
```

```python
import functools

import jax
import jax.numpy as jnp
from jax import lax
from jax.experimental import pallas as pl
from jax.experimental.pallas import tpu as pltpu
from jax.sharding import PartitionSpec as P

F32, BF16 = jnp.float32, jnp.bfloat16
MESH = pl.DeviceIdType.MESH
D, HEADS, HEAD, TOK, CH, FF = 1024, 16, 64, 64, 64, 4096
ROWS = 256
RB = 16
STAGES = 4
INV_D = 1.0 / D
GC0 = 0.7978845608028654
GC1 = GC0 * 0.044715
LOG2E = 1.4426950408889634
TRAIL, LAG, LEAD = 3, 4, 3
VMEM_LIMIT = 45 << 20


def dot(a, b):
    return jnp.dot(a, b, preferred_element_type=F32)


def merge(first, second):
    total_a = sum(w for w, _ in first)
    total_b = sum(w for w, _ in second)
    ia = ib = 0
    done_a = done_b = 0.0
    while ia < len(first) or ib < len(second):
        take_a = ib >= len(second) or (ia < len(first) and done_a / total_a <= done_b / total_b)
        if take_a:
            w, piece = first[ia]
            ia, done_a = ia + 1, done_a + w
        else:
            w, piece = second[ib]
            ib, done_b = ib + 1, done_b + w
        piece()


def wide(ref, rows=slice(None), tiles=None):
    tiles = range(ref.shape[0]) if tiles is None else tiles
    return jnp.concatenate([ref[c, rows, :] for c in tiles], axis=1)


def put(ref, first, rows, value):
    for c in range(value.shape[1] // 128):
        ref[first + c, rows, :] = value[:, c * 128:(c + 1) * 128].astype(BF16)


def kernel(steps, chunks,
           x_hbm, warm_hbm, lat_hbm, qkv_hbm, o_hbm, up_hbm, down_hbm, out_hbm, mods_hbm, alpha, beta,
           xf, buf,
           wlat, wq, wk, wv, wo, wup, wdown, wout_t, mods_t, mods,
           xb, ebuf,
           h_a, h_n, h_b, u_a, u_b, k_s, qv_s, p_s, o_s, hid,
           s_sem, lat_sem, q_sem, k_sem, v_sem, o_sem, up_sem, down_sem,
           warm_sem, st_send, st_recv, x_send, x_recv, xo_send, xo_recv):
    st = lax.axis_index('stage')
    last = STAGES - 1
    total = steps * chunks

    def tiled(src, first, dst, sem):
        return [pltpu.make_async_copy(src.at[:, pl.ds(first + c * 128, 128)], dst.at[c], sem.at[c]) for c in range(dst.shape[0])]

    ld_s = [pltpu.make_async_copy(src, dst, s_sem.at[n])
            for n, (src, dst) in enumerate(((x_hbm, xf), (mods_hbm, mods_t), (out_hbm, wout_t)))]
    ld_lat = tiled(lat_hbm, 0, wlat, lat_sem)
    ld_qkv = tiled(qkv_hbm, 0, wq, q_sem) + tiled(qkv_hbm, D, wk, k_sem) + tiled(qkv_hbm, 2 * D, wv, v_sem)
    ld_o = tiled(o_hbm, 0, wo, o_sem)
    ld_up = tiled(up_hbm, 0, wup, up_sem)
    ld_down = tiled(down_hbm, 0, wdown, down_sem)
    warm_stage = jnp.maximum(st - 1, 0)

    def warm_copy(c):
        return pltpu.make_async_copy(warm_hbm.at[warm_stage, c], buf.at[c], warm_sem.at[c])

    for ld in ld_s + ld_lat:
        ld.start()
    warm_copy(0).start()
    for ld in ld_qkv + ld_o:
        ld.start()
    warm_copy(1).start()

    barrier = pltpu.get_barrier_semaphore()
    for k in range(1, STAGES):
        pl.semaphore_signal(barrier, inc=1, device_id={'stage': lax.rem(st + k, STAGES)}, device_id_type=MESH)

    def stale_copy(k):
        nxt = jnp.minimum(st + 1, last)
        return pltpu.make_async_remote_copy(
            src_ref=buf.at[k], dst_ref=buf.at[k + chunks], send_sem=st_send.at[k], recv_sem=st_recv.at[k],
            device_id={'stage': nxt}, device_id_type=MESH)

    def latent_copy(k, dst):
        return pltpu.make_async_remote_copy(
            src_ref=xb.at[k + chunks], dst_ref=xb.at[k + chunks], send_sem=x_send.at[dst, k], recv_sem=x_recv.at[k],
            device_id={'stage': dst}, device_id_type=MESH)

    def xout_copy(c, dst):
        return pltpu.make_async_remote_copy(
            src_ref=xf.at[c], dst_ref=xf.at[c], send_sem=xo_send.at[dst, c], recv_sem=xo_recv.at[c],
            device_id={'stage': dst}, device_id_type=MESH)

    def wait_inputs(k):
        @pl.when(k < chunks)
        def _():
            warm_copy(k).wait()

        @pl.when(jnp.logical_and(k >= chunks, st > 0))
        def _():
            stale_copy(k - chunks).wait_recv()

        @pl.when(jnp.logical_and(k >= chunks, st < last))
        def _():
            latent_copy(k - chunks, 0).wait_recv()

    def send_stage(k):
        @pl.when(jnp.logical_and(k < total - chunks, st < last))
        def _():
            stale_copy(k).start()

    def finish_latent(k, slot):
        step, c = lax.div(k, chunks), lax.rem(k, chunks)

        @pl.when(st == last)
        def _():
            x_new = alpha[step] * xf[c] + beta[step] * ebuf[slot]
            xf[c] = x_new

            @pl.when(step < steps - 1)
            def _():
                xb[k + chunks] = x_new.astype(BF16)
                for dst in range(last):
                    latent_copy(k, dst).start()

            @pl.when(step == steps - 1)
            def _():
                for dst in range(last):
                    xout_copy(c, dst).start()

    lane = lax.broadcasted_iota(jnp.int32, (HEAD, 4 * TOK), 1)
    left = lax.rem(lane, 2 * TOK) < TOK
    zero_q = jnp.zeros((HEAD, 2 * TOK), BF16)
    blocks = [slice(r * RB, (r + 1) * RB) for r in range(ROWS // RB)]

    def norm(h, dst, rows, step, scale, shift):
        mean = jnp.sum(h, axis=-1, keepdims=True) * INV_D
        cen = h - mean
        var = jnp.sum(cen * cen, axis=-1, keepdims=True) * INV_D
        put(dst, 0, rows, cen * lax.rsqrt(var + 1e-6) * mods[step, scale:scale + 1, :] + mods[step, shift:shift + 1, :])

    def latent_pieces(k):
        def latent(n):
            cols = slice(n * 256, (n + 1) * 256)
            stale = jnp.where(st > 0, buf[k, :, cols].astype(F32), 0.0)
            h_a[:, cols] = stale + dot(xb[k], wide(wlat, tiles=(2 * n, 2 * n + 1)))
        return [(64, functools.partial(latent, n)) for n in range(4)]

    def norm1_pieces(k):
        step = lax.div(k, chunks)

        def norm1(rows):
            norm(h_a[rows, :], u_a, rows, step, 1, 0)
        return [(40, functools.partial(norm1, rows)) for rows in blocks]

    def proj_pieces():
        def proj_k(n):
            put(k_s, 2 * n, slice(None), dot(wide(u_a), wide(wk, tiles=(2 * n, 2 * n + 1))))

        def proj_qv(n):
            part, w = (0, wq) if n < 4 else (D, wv)
            n = n % 4
            val = dot(wide(u_a), wide(w, tiles=(2 * n, 2 * n + 1))).astype(BF16).T
            put(qv_s, 0, slice(part + n * 256, part + (n + 1) * 256), val)
        return [(256, functools.partial(proj_qv, n)) for n in range(8)] + [(256, functools.partial(proj_k, n)) for n in range(4)]

    h2 = 2 * TOK

    def attend_pieces():
        groups = [(p, hp) for p in range(ROWS // h2) for hp in range(HEADS // 2)]

        def scores(g):
            p, hp = groups[g]
            r0, l0 = hp * 2 * HEAD, p * h2
            q0 = qv_s[p, r0:r0 + HEAD, :]
            q1 = qv_s[p, r0 + HEAD:r0 + 2 * HEAD, :]
            rhs = jnp.concatenate([jnp.concatenate([q0, zero_q], axis=1), jnp.concatenate([zero_q, q1], axis=1)], axis=0)
            both = dot(k_s[hp, l0:l0 + h2, :], rhs)
            s = jnp.where(left, both[:TOK], both[TOK:])
            e = jnp.exp2((s - jnp.max(s, axis=0, keepdims=True)) * (HEAD ** -0.5 * LOG2E))
            pr = e * (1.0 / jnp.sum(e, axis=0, keepdims=True))
            put(p_s, 4 * g, slice(None), jnp.where(left, pr, 0.0))
            put(p_s, 4 * g + 2, slice(None), jnp.where(left, 0.0, pr))

        def mix(g):
            p, hp = groups[g]
            r0, l0 = D + hp * 2 * HEAD, p * h2
            rhs = jnp.concatenate([
                jnp.concatenate([p_s[4 * g], zero_q], axis=1), jnp.concatenate([p_s[4 * g + 2], zero_q], axis=1),
                jnp.concatenate([zero_q, p_s[4 * g + 1]], axis=1), jnp.concatenate([zero_q, p_s[4 * g + 3]], axis=1)], axis=0)
            v = jnp.concatenate([qv_s[p, r0:r0 + HEAD, :], qv_s[p, r0 + HEAD:r0 + 2 * HEAD, :]], axis=1)
            ot = dot(v, rhs)
            ot = jnp.concatenate([ot[:, :h2], ot[:, h2:]], axis=0)
            o_s[hp, l0:l0 + h2, :] = ot.astype(BF16).T

        return ([functools.partial(scores, g) for g in range(len(groups))],
                [functools.partial(mix, g) for g in range(len(groups))])

    def attend_up():
        scores, mixes = attend_pieces()
        ups = up_pieces()
        done_s = done_m = 0
        for n, (_, up) in enumerate(ups):
            up()
            while done_s < min(len(scores), (n + 1) * len(scores) / (len(ups) - TRAIL)):
                scores[done_s]()
                done_s += 1
            while done_m < min(len(mixes), done_s - LAG if n < len(ups) - TRAIL else (n + 1 - LEAD) * len(mixes) / (len(ups) - LEAD)):
                mixes[done_m]()
                done_m += 1

    def proj_o_pieces(k):
        step = lax.div(k, chunks)

        def proj_o(n):
            cols = slice(n * 256, (n + 1) * 256)
            h_n[:, cols] = h_a[:, cols] + mods[step, 2:3, cols] * dot(wide(o_s), wide(wo, tiles=(2 * n, 2 * n + 1)))
        return [(256, functools.partial(proj_o, n)) for n in range(4)]

    def norm2_pieces(k):
        step = lax.div(k, chunks)
        return [(40, lambda rows=rows: norm(h_n[rows, :], u_b, rows, step, 4, 3)) for rows in blocks]

    def keep_pieces():
        def keep(rows):
            h_b[rows, :] = h_n[rows, :]
        return [(20, functools.partial(keep, rows)) for rows in blocks]

    def up_pieces():
        def up(n):
            z = dot(wide(u_b), wide(wup, tiles=(2 * n, 2 * n + 1)))
            half = 0.5 * z
            t = jnp.tanh(z * (GC0 + GC1 * (z * z)))
            put(hid, 2 * n, slice(None), half + half * t)
        return [(256, functools.partial(up, n)) for n in range(FF // 256)]

    def down_pieces(k):
        step = lax.div(k, chunks)

        def down(n):
            cols = slice(n * 256, (n + 1) * 256)
            y = dot(wide(hid), wide(wdown, tiles=(2 * n, 2 * n + 1)))
            buf[k, :, cols] = (h_b[:, cols] + mods[step, 5:6, cols] * y).astype(BF16)
        return [(1024, functools.partial(down, n)) for n in range(4)]

    def noise(k, slot):
        ebuf[slot] = lax.dot_general(wout_t[...], buf[k], (((1,), (1,)), ((), ())), preferred_element_type=F32).T

    def run(*lists):
        for pieces in lists:
            for _, piece in pieces:
                piece()

    def norms(second, first):
        out = []
        for n in range(len(blocks)):
            out += second[n:n + 1] + first[n:n + 1]
        return out

    def finish(k, ahead, down):
        run(proj_o_pieces(k))
        if ahead is not None:
            run(latent_pieces(ahead))
        run(down[:2])
        if ahead is None:
            run(norm2_pieces(k), down[2:])
        else:
            run(norms(norm2_pieces(k), norm1_pieces(ahead)))
            merge(proj_pieces(), down[2:]) if down else run(proj_pieces())

    for ld in ld_s + ld_lat:
        ld.wait()
    for c in range(chunks):
        xb[c] = xf[c].astype(BF16)
    for step in range(steps):
        for j in range(6):
            row = mods_t[step * 6 + j]
            mods[step, j:j + 1, :] = row + 1.0 if j in (1, 4) else row
    wait_inputs(0)
    run(latent_pieces(0), norm1_pieces(0))
    for ld in ld_qkv:
        ld.wait()
    for ld in ld_up + ld_down:
        ld.start()
    for c in range(2, chunks):
        warm_copy(c).start()
    run(proj_pieces())
    for pieces in attend_pieces():
        for piece in pieces:
            piece()
    for ld in ld_o:
        ld.wait()
    wait_inputs(1)
    finish(0, 1, [])
    run(keep_pieces())
    for ld in ld_up + ld_down:
        ld.wait()
    pl.semaphore_wait(barrier, STAGES - 1)

    def body(i, ahead, slot):
        attend_up()
        noise(jnp.maximum(i - 1, 0), slot)
        finish(i + 1, ahead, down_pieces(i))
        run(keep_pieces())

    @pl.loop(0, (total - 2) // 2)
    def _(pair):
        i = 2 * pair
        wait_inputs(i + 2)
        wait_inputs(i + 3)
        body(i, i + 2, 0)
        body(i + 1, i + 3, 1)
        send_stage(i)
        send_stage(i + 1)

        @pl.when(i > 0)
        def _():
            finish_latent(i - 1, 0)
        finish_latent(i, 1)

    body(total - 2, None, 0)
    finish_latent(total - 3, 0)
    noise(total - 2, 1)
    finish_latent(total - 2, 1)
    run(up_pieces(), down_pieces(total - 1))
    noise(total - 1, 0)
    finish_latent(total - 1, 0)

    @pl.when(st < last)
    def _():
        @pl.loop(0, total - chunks)
        def _(k):
            stale_copy(k).wait_send()

        for c in range(chunks):
            xout_copy(c, 0).wait_recv()

    @pl.when(st == last)
    def _():
        @pl.loop(0, total - chunks)
        def _(k):
            for dst in range(last):
                latent_copy(k, dst).wait_send()

        for c in range(chunks):
            for dst in range(last):
                xout_copy(c, dst).wait_send()


def solution(mesh):
    def program(x_init, h_warm, w_lat, w_qkv, w_o, w_up, w_down, w_out, ada_mods, alpha_coef, beta_coef):
        batch, steps = x_init.shape[0], ada_mods.shape[0]
        chunks = batch * TOK // ROWS
        total = steps * chunks
        any_spec = pl.BlockSpec(memory_space=pl.ANY)
        vmem_spec = pl.BlockSpec(memory_space=pltpu.VMEM)
        smem = pl.BlockSpec(memory_space=pltpu.SMEM)
        dma = pltpu.SemaphoreType.DMA
        vb, vf = (lambda *shape: pltpu.VMEM(shape, BF16)), (lambda *shape: pltpu.VMEM(shape, F32))
        flops = 2 * total * ROWS * D * D * 13
        x_out, h_all = pl.pallas_call(
            functools.partial(kernel, steps, chunks),
            out_shape=(pltpu.VMEM((chunks, ROWS, CH), F32), pltpu.VMEM((total, ROWS, D), BF16)),
            in_specs=[any_spec] * 9 + [smem] * 2,
            out_specs=(vmem_spec, vmem_spec),
            scratch_shapes=[
                vb(8, CH, 128), vb(8, D, 128), vb(8, D, 128), vb(8, D, 128), vb(8, D, 128), vb(32, D, 128), vb(8, FF, 128),
                vb(CH, D), vf(6 * steps, 1, D), vf(steps, 6, D),
                vb(total, ROWS, CH), vf(2, ROWS, CH),
                vf(ROWS, D), vf(ROWS, D), vf(ROWS, D),
                vb(8, ROWS, 128), vb(8, ROWS, 128), vb(8, ROWS, 128), vb(2, 2 * D, 128), vb(64, TOK, 128), vb(8, ROWS, 128), vb(32, ROWS, 128),
                dma((3,)), dma((8,)), dma((8,)), dma((8,)), dma((8,)), dma((8,)), dma((32,)), dma((8,)),
                dma((chunks,)), dma((total - chunks,)), dma((total - chunks,)),
                dma((STAGES - 1, total - chunks)), dma((total - chunks,)), dma((STAGES - 1, chunks)), dma((chunks,)),
            ],
            compiler_params=pltpu.CompilerParams(
                collective_id=0, has_side_effects=True, vmem_limit_bytes=VMEM_LIMIT),
            cost_estimate=pl.CostEstimate(flops=flops, bytes_accessed=40 << 20, transcendentals=0),
        )(x_init.reshape(chunks, ROWS, CH), h_warm.reshape(STAGES - 1, chunks, ROWS, D),
          w_lat[0], w_qkv[0], w_o.reshape(D, D), w_up[0], w_down[0], w_out.T, ada_mods.reshape(steps * 6, 1, D), alpha_coef, beta_coef)
        return x_out.reshape(x_init.shape), h_all[total - chunks:].reshape(1, batch, TOK, D)

    return jax.shard_map(program, mesh=mesh,
                         in_specs=(P('data'), P(None, 'data'), P('stage'), P('stage'), P('stage'), P('stage'), P('stage'), P(), P(None, 'stage'), P(), P()),
                         out_specs=(P('data'), P('stage', 'data')), check_vma=False)
```
